32 devices in a mesh: seq: 16 (over z, y, x), mp: 2 (over core).
Axes of the slice: x: 2, y: 2, z: 4, core: 2. Of those that a mesh axis runs over, the one named last changes fastest.
Arguments:
- encoded: bfloat16 [4096, 1152], P('seq'), may hold values from -6 to 6
- frame_tokens: int32 [16, 2], P('seq'), may hold values from 1 to 196, 256 in all within a row
- slot_owner: int32 [32], replicated, may hold values from 0 to 15, as said below
- w_in: bfloat16 [1152, 3584], P('seq', 'mp'), may hold values from -0.1875 to 0.1875
- b_in: bfloat16 [3584], P('mp'), may hold values from -3 to 3
- w_out: bfloat16 [3584, 3584], P('seq', 'mp'), may hold values from -0.09375 to 0.09375
- b_out: bfloat16 [3584], P('mp'), may hold values from -6.4 to 6.4
- norm_gain: bfloat16 [3584], replicated, may hold values from 0.5 to 1.5
- w_key: bfloat16 [3584, 512], P('seq', 'mp'), may hold values from -0.09375 to 0.09375
- b_key: bfloat16 [512], P('mp'), may hold values from -3 to 3
- w_value: bfloat16 [3584, 512], P('seq', 'mp'), may hold values from -0.09375 to 0.09375
- b_value: bfloat16 [512], P('mp'), may hold values from -3 to 3
Outputs:
- keys: bfloat16 [4096, 512], P('seq', 'mp')
- values: bfloat16 [4096, 512], P('seq', 'mp')
The draws below stay inside these ranges and needn't reach their ends.
Inputs may be any that keep to these rules, and one draw needn't show every extreme that they name: `slot_owner`: each shard index 0 to 15 appears exactly twice. `frame_tokens`: each row sums to 256.
All inputs are finite; a program needn't handle non-finite values.
Results may differ from the reference program's by a relative error of at most 0.01.
Values may be sent and summed in bfloat16 or wider, within the bound.
No kernel may reach another device: no remote copies, remote signals or barrier semaphores. Data moves between devices by JAX's collectives and lax.ppermute only.
A program may use at most 128 MiB of HBM per device.

```python
import math
import jax
import jax.numpy as jnp
import numpy as np
from jax import lax

ENC = 1152
PHID = 3584
D = 3584
KVH = 4
HEAD = 128
TSEC = 16
PATCH = 196
TOK_DEV = 256
FR_DEV = 2
TOKENS = 4096
N_SEQ = 16


def draw_slot_owner(key, part):
    return (jax.random.permutation(key, 2 * N_SEQ) // 2).astype(jnp.int32)


def draw_b_out(key, part):
    ramp = 0.2 + 1.4 * jnp.arange(D, dtype=jnp.float32) / D
    base = jax.random.truncated_normal(key, -4.0, 4.0, (D,), jnp.float32)
    return (base * ramp).astype(jnp.bfloat16)


def level_of(own_key, shape, pieces, least, high):
    gain, own = 1.0, jax.random.fold_in(own_key, 6)
    for position, blocks in pieces:
        draws = jnp.exp(jax.random.uniform(jax.random.fold_in(own, position), (blocks,), jnp.float32, least / len(pieces), high / len(pieces)))
        gain = gain * jnp.repeat(draws, shape[position] // blocks).reshape([-1 if axis == position else 1 for axis in range(len(shape))])
    return gain


def profile(amount, total, limit, slope):
    portions = [(1 << 20) // math.isqrt(grade ** slope) + 1 for grade in range(2, amount + 1)]
    surplus, holding = total - limit - (amount - 1), [1] * (amount - 1)
    while surplus > 0:
        movable = [i for i in range(amount - 1) if holding[i] < limit]
        mass, left = sum([portions[i] for i in movable]), surplus
        for i in movable:
            more = min(limit - holding[i], max(1, left * portions[i] // mass), surplus)
            holding[i] = holding[i] + more
            surplus = surplus - more
    return np.array([limit] + holding)


def ragged(rng, count, total, bound, slope):
    if count == 2:
        one = jax.random.randint(rng, (), max(1, total - bound), min(bound, total - 1) + 1)
        return jnp.stack([one, total - one])
    sizes = jnp.asarray(profile(count, total, bound, slope), jnp.int32)
    pairs = (count - 1) // 2
    donor, receiver = sizes[1:1 + 2 * pairs:2], sizes[2:2 + 2 * pairs:2]
    margin = jnp.minimum(donor - 1, bound - receiver)
    moved = jax.random.randint(jax.random.fold_in(rng, 1), (pairs,), 0, 1 << 20) % (margin + 1)
    sizes = sizes.at[1:1 + 2 * pairs:2].set(donor - moved).at[2:2 + 2 * pairs:2].set(receiver + moved)
    return sizes[jax.random.permutation(jax.random.fold_in(rng, 2), count)]


def gaussian(own_key, shape, width, reach, split=(), kind=jnp.bfloat16):
    result = width * jax.random.normal(own_key, shape, jnp.float32)
    if split:
        result = result * level_of(own_key, shape, split, -0.22, 0.18)
    return jnp.clip(result, -reach, reach).astype(kind)


def setup_inputs(seed: int = 0) -> dict:
    streams_of = jax.random.split(jax.random.key(seed), 13)
    return {
        "encoded": gaussian(streams_of[0], (TOKENS, ENC), 1.0, 6.0, ((0, 16),)),
        "frame_tokens": jax.vmap(lambda own: ragged(own, FR_DEV, TOK_DEV, PATCH, 1))(jax.random.split(streams_of[1], N_SEQ)).reshape((N_SEQ, FR_DEV)).astype(jnp.int32),
        "slot_owner": draw_slot_owner(jax.random.fold_in(streams_of[12], 71), 0),
        "w_in": gaussian(streams_of[3], (ENC, PHID), ENC ** -0.5, 0.1875, ((0, 16), (1, 2))),
        "b_in": gaussian(streams_of[4], (PHID,), 0.5, 3.0, ((0, 2),)),
        "w_out": gaussian(streams_of[5], (PHID, D), PHID ** -0.5, 0.09375, ((0, 16), (1, 2))),
        "b_out": draw_b_out(jax.random.fold_in(streams_of[12], 71), 0),
        "norm_gain": jnp.clip(1.0 + 0.1 * jax.random.normal(streams_of[7], (D,), jnp.float32), 0.5, 1.5).astype(jnp.bfloat16),
        "w_key": gaussian(streams_of[8], (D, KVH * HEAD), D ** -0.5, 0.09375, ((0, 16), (1, 2))),
        "b_key": gaussian(streams_of[9], (KVH * HEAD,), 0.5, 3.0, ((0, 2),)),
        "w_value": gaussian(streams_of[10], (D, KVH * HEAD), D ** -0.5, 0.09375, ((0, 16), (1, 2))),
        "b_value": gaussian(streams_of[11], (KVH * HEAD,), 0.5, 3.0, ((0, 2),)),
    }


norm_eps = 1e-06
rope_base = 1000000.0

def rotate(linear, frame_ids, offsets):
    pairs = HEAD // 2
    pair_index = jnp.arange(pairs)
    inverse = jnp.power(jnp.float32(rope_base), -2.0 * pair_index.astype(jnp.float32) / HEAD)
    chosen = jnp.where(pair_index[None, :] < TSEC, frame_ids[:, None], offsets[:, None]).astype(jnp.float32)
    angles = chosen * inverse[None, :]
    cosine = jnp.cos(angles)[:, None, :]
    sine = jnp.sin(angles)[:, None, :]
    shaped = linear.reshape(linear.shape[0], -1, HEAD)
    first_half = shaped[..., :pairs]
    second_half = shaped[..., pairs:]
    turned = jnp.concatenate([first_half * cosine - second_half * sine, second_half * cosine + first_half * sine], axis=-1)
    return turned.reshape(linear.shape)

def positions(local_rows, counts):
    frame_ends = jnp.cumsum(counts)
    finished = frame_ends[None, :] <= local_rows[:, None]
    frame_local = lax.optimization_barrier(jnp.sum(finished.astype(jnp.int32), axis=1))
    frame_start = lax.optimization_barrier(jnp.sum(jnp.where(finished, counts[None, :], 0), axis=1))
    return (frame_local, local_rows - frame_start)

def reference(encoded, frame_tokens, slot_owner, w_in, b_in, w_out, b_out, norm_gain, w_key, b_key, w_value, b_value):
    frames_here = frame_tokens.shape[1]

    def encode_block(operands):
        rows_in, counts, device_number = operands
        pre = jnp.dot(rows_in, w_in, preferred_element_type=jnp.float32) + b_in.astype(jnp.float32)
        hidden = jax.nn.gelu(pre, approximate=False).astype(jnp.bfloat16)
        projected = (jnp.dot(hidden, w_out, preferred_element_type=jnp.float32) + b_out.astype(jnp.float32)).astype(jnp.bfloat16)
        wide = projected.astype(jnp.float32)
        inv_rms = lax.rsqrt(lax.optimization_barrier(jnp.mean(wide * wide, axis=1)) + norm_eps)
        normed = (wide * inv_rms[:, None] * norm_gain.astype(jnp.float32)).astype(jnp.bfloat16)
        key_linear = jnp.dot(normed, w_key, preferred_element_type=jnp.float32) + b_key.astype(jnp.float32)
        value_rows = (jnp.dot(normed, w_value, preferred_element_type=jnp.float32) + b_value.astype(jnp.float32)).astype(jnp.bfloat16)
        local_rows = jnp.arange(TOK_DEV, dtype=jnp.int32)
        frame_local, offsets = positions(local_rows, counts)
        frame_ids = device_number * frames_here + frame_local
        key_rows = rotate(key_linear, frame_ids, offsets).astype(jnp.bfloat16)
        return (key_rows, value_rows)
    blocks = encoded.reshape(N_SEQ, TOK_DEV, encoded.shape[1])
    numbers = jnp.arange(N_SEQ, dtype=jnp.int32)
    key_blocks, value_blocks = lax.map(encode_block, (blocks, frame_tokens, numbers))
    key_all = key_blocks.reshape(TOKENS, -1)
    value_all = value_blocks.reshape(TOKENS, -1)
    slot_order = jnp.argsort(slot_owner, stable=True).astype(jnp.int32)
    out_rows = jnp.arange(TOKENS, dtype=jnp.int32)
    shard = out_rows // TOK_DEV
    remain = out_rows % TOK_DEV
    source = remain // 2 * (2 * N_SEQ) + slot_order[2 * shard + remain % 2]
    return (jnp.take(key_all, source, axis=0), jnp.take(value_all, source, axis=0))
```

```python
import jax
import jax.numpy as jnp
from jax import lax
from jax.sharding import PartitionSpec as P

HEAD = 128
TSEC = 16
LANE = 128

norm_eps = 1e-06
rope_base = 1000000.0


f32 = jnp.float32
bf16 = jnp.bfloat16


def rotate(linear, frame_ids, offsets):
    pairs = HEAD // 2
    pair_index = jnp.arange(pairs)
    inverse = jnp.power(f32(rope_base), -2.0 * pair_index.astype(f32) / HEAD)
    chosen = jnp.where(pair_index[None, :] < TSEC, frame_ids[:, None], offsets[:, None])
    angles = chosen * inverse[None, :]
    cosine = jnp.cos(angles)
    sine = jnp.sin(angles)
    turned = []
    for head in range(linear.shape[1] // HEAD):
        first = linear[:, head * HEAD : head * HEAD + pairs]
        second = linear[:, head * HEAD + pairs : (head + 1) * HEAD]
        turned += [first * cosine - second * sine, second * cosine + first * sine]
    return jnp.concatenate(turned, axis=1)


def swap(x, bit, count):
    return lax.ppermute(x, "seq", [(i, i ^ (1 << bit)) for i in range(count)])


def swap_core(x):
    return lax.ppermute(x, "mp", [(0, 1), (1, 0)])


def join(own, other, bit, axis):
    low = jnp.stack([own, other], axis=axis)
    high = jnp.stack([other, own], axis=axis)
    return jnp.where(bit == 1, high, low)


def spread(block, bits, held, values, count):
    held = list(held)
    for bit in bits:
        other = swap(block, bit, count)
        axis = sum(1 for b in held if b > bit)
        block = join(block, other, values[bit], axis)
        held.insert(axis, bit)
    return block.reshape(-1, block.shape[-1])


def cut_point(width):
    return (width // LANE + 1) // 2 * LANE


def shards(
    encoded,
    frame_tokens,
    slot_owner,
    w_in,
    b_in,
    w_out,
    b_out,
    norm_gain,
    w_key,
    b_key,
    w_value,
    b_value,
):
    seq = lax.axis_size("seq")
    index = lax.axis_index("seq")
    core = lax.axis_index("mp")
    depth = seq.bit_length() - 1
    assert seq == 1 << depth and lax.axis_size("mp") == 2
    values = [(index >> b) & 1 for b in range(depth)]
    top, mate = depth - 1, depth - 2
    lows = list(range(depth - 2))
    orders = (lows, lows[::-1])
    side = values[mate]

    def halves(w):
        half = w.shape[1] // 2
        left, right = w[:, :half], w[:, half:]
        return jnp.where(side == 1, right, left), jnp.where(side == 1, left, right)

    def gather(w):
        keep, give = halves(w)
        pair = join(keep, swap(give, mate, seq), side, 0)
        quad = join(pair, swap(pair, top, seq), values[top], 0)
        cut = cut_point(keep.shape[1])
        parts = (quad[..., :cut], quad[..., cut:])
        return [spread(p, o, (top, mate), values, seq) for p, o in zip(parts, orders)]

    rows, width = encoded.shape
    slots = 2 * seq
    rounds = rows // slots
    counts = frame_tokens[0]
    local = jnp.arange(rows, dtype=jnp.int32)
    ends = jnp.cumsum(counts)
    done = ends[None, :] <= local[:, None]
    frame = index * counts.shape[0] + jnp.sum(done.astype(jnp.int32), axis=1)
    offset = local - jnp.sum(jnp.where(done, counts[None, :], 0), axis=1)
    marks = jnp.stack([frame // 256, frame % 256, offset // 256, offset % 256], axis=1)
    marks = jnp.pad(marks.astype(bf16), ((0, 0), (0, LANE - 4)))
    tiles = width // LANE
    wide = (tiles + 1) // 2 * LANE
    first = encoded[:, :wide]
    second = jnp.concatenate([marks, encoded[:, wide:]], axis=1)
    if second.shape[1] < wide + (LANE if tiles % 2 == 0 else 0):
        raise ValueError("width")
    if tiles % 2 == 0:
        first = jnp.pad(first, ((0, 0), (0, LANE)))
    payload = jnp.where(core == 1, second, first)
    order = jnp.argsort(slot_owner, stable=True).astype(jnp.int32)
    pick = (
        jnp.arange(rounds, dtype=jnp.int32)[None, :, None] * slots + order.reshape(seq, 1, 2)
    ).reshape(-1)
    moved = jnp.take(payload, pick, axis=0).reshape(seq, 2 * rounds, -1)
    arrived = lax.all_to_all(moved, "seq", split_axis=0, concat_axis=0, tiled=True)
    arrived = arrived.reshape(rows, -1)
    both = join(arrived, swap(arrived, mate, seq), side, 0).reshape(2 * rows, -1)
    ready = join(both, swap_core(both), core, 0)
    tokens = jnp.concatenate([ready[0, :, :wide], ready[1, :, LANE:]], axis=1)
    own_marks = lax.dynamic_slice_in_dim(ready[1, :, :4], side * rows, rows, 0).astype(f32)
    frame_ids = own_marks[:, 0] * 256 + own_marks[:, 1]
    offsets = own_marks[:, 2] * 256 + own_marks[:, 3]

    own_b_in, _ = halves(b_in[None, :])
    cut = cut_point(own_b_in.shape[1])
    hidden = []
    for w, b in zip(gather(w_in), (own_b_in[:, :cut], own_b_in[:, cut:])):
        pre = jnp.dot(tokens, w, preferred_element_type=f32) + b.astype(f32)
        part = jax.nn.gelu(pre, approximate=False).astype(bf16)
        hidden.append(part)
    quarter = jnp.concatenate(hidden, axis=1)
    pair_hidden = join(quarter, swap(quarter, mate, seq), side, 0)
    all_hidden = join(pair_hidden, swap_core(pair_hidden), core, 0)
    all_hidden = all_hidden.reshape((4,) + quarter.shape)

    kv = jnp.concatenate([w_key, w_value], axis=1)
    kv_row = join(kv, swap_core(kv), core, 1).reshape(kv.shape[0], -1)
    pairs = [
        (2 * i + h, 2 * (i ^ (1 << top)) + h) for i in range(seq) for h in range(2) if i >> top == h
    ]
    far = lax.ppermute(kv_row, ("seq", "mp"), pairs)
    kv_row = jnp.where(values[top] == core, kv_row, far)
    kv_cut = kv_row.shape[1] // 2
    kv_full = jnp.concatenate(
        [
            spread(p, o, (), values, seq)
            for p, o in zip((kv_row[:, :kv_cut], kv_row[:, kv_cut:]), orders)
        ],
        axis=1,
    )

    own_b_out, _ = halves(b_out[None, :])
    span = own_b_out.shape[1]
    gain = lax.dynamic_slice_in_dim(norm_gain, (2 * core + side) * span, span)[None, :]
    squares = 0.0
    partial = 0.0
    start = 0
    for w in gather(w_out):
        stop = start + w.shape[1]
        blocks = w.reshape(4, -1, w.shape[1])
        summed = own_b_out[:, start:stop].astype(f32)
        for q in range(4):
            summed = summed + jnp.dot(all_hidden[q], blocks[q], preferred_element_type=f32)
        projected = summed.astype(bf16).astype(f32)
        squares = squares + jnp.sum(projected * projected, axis=1)
        scaled = (projected * gain[:, start:stop].astype(f32)).astype(bf16)
        partial = partial + jnp.dot(scaled, kv_full[start:stop], preferred_element_type=f32)
        start = stop

    squares = squares + swap_core(squares)
    squares = squares.reshape(2, rows)
    other_squares = swap(jnp.where(side == 1, squares[0], squares[1]), mate, seq)
    squares = jnp.where(side == 1, squares[1], squares[0]) + other_squares
    inv_rms = lax.rsqrt(squares / norm_gain.shape[0] + norm_eps)[:, None]

    keep = jnp.where(core == 1, partial[:, kv_cut:], partial[:, :kv_cut])
    give = jnp.where(core == 1, partial[:, :kv_cut], partial[:, kv_cut:])
    summed = keep + swap_core(give)
    keep = jnp.where(side == 1, summed[rows:], summed[:rows])
    give = jnp.where(side == 1, summed[:rows], summed[rows:])
    summed = keep + swap(give.astype(bf16), mate, seq).astype(f32)
    linear = summed * inv_rms
    half = w_key.shape[1]
    keys = rotate(linear[:, :half] + b_key.astype(f32), frame_ids, offsets).astype(bf16)
    vals = (linear[:, half:] + b_value.astype(f32)).astype(bf16)
    return keys, vals


def solution(mesh):
    return jax.shard_map(
        shards,
        mesh=mesh,
        in_specs=(
            P("seq", None),
            P("seq", None),
            P(),
            P("seq", "mp"),
            P("mp"),
            P("seq", "mp"),
            P("mp"),
            P(),
            P("seq", "mp"),
            P("mp"),
            P("seq", "mp"),
            P("mp"),
        ),
        out_specs=(P("seq", "mp"), P("seq", "mp")),
        check_vma=False,
    )
```

```python
import jax
import jax.numpy as jnp
from jax import lax
from jax.experimental import pallas as pl
from jax.experimental.pallas import tpu as pltpu
from jax.sharding import PartitionSpec as P

HEAD = 128
TSEC = 16
LANE = 128

norm_eps = 1e-06
rope_base = 1000000.0


f32 = jnp.float32
bf16 = jnp.bfloat16


def rotate(linear, frame_ids, offsets):
    pairs = HEAD // 2
    pair_index = jnp.arange(pairs)
    inverse = jnp.power(f32(rope_base), -2.0 * pair_index.astype(f32) / HEAD)
    chosen = jnp.where(pair_index[None, :] < TSEC, frame_ids[:, None], offsets[:, None])
    angles = chosen * inverse[None, :]
    cosine = jnp.cos(angles)
    sine = jnp.sin(angles)
    turned = []
    for head in range(linear.shape[1] // HEAD):
        first = linear[:, head * HEAD : head * HEAD + pairs]
        second = linear[:, head * HEAD + pairs : (head + 1) * HEAD]
        turned += [first * cosine - second * sine, second * cosine + first * sine]
    return jnp.concatenate(turned, axis=1)


def swap(x, bit, count):
    return lax.ppermute(x, "seq", [(i, i ^ (1 << bit)) for i in range(count)])


def swap_core(x):
    return lax.ppermute(x, "mp", [(0, 1), (1, 0)])


def join(own, other, bit, axis):
    low = jnp.stack([own, other], axis=axis)
    high = jnp.stack([other, own], axis=axis)
    return jnp.where(bit == 1, high, low)


def spread(block, bits, held, values, count):
    held = list(held)
    for bit in bits:
        other = swap(block, bit, count)
        axis = sum(1 for b in held if b > bit)
        block = join(block, other, values[bit], axis)
        held.insert(axis, bit)
    return block.reshape(-1, block.shape[-1])


def cut_point(width):
    return (width // LANE + 1) // 2 * LANE


def shards(
    encoded,
    frame_tokens,
    slot_owner,
    w_in,
    b_in,
    w_out,
    b_out,
    norm_gain,
    w_key,
    b_key,
    w_value,
    b_value,
):
    seq = lax.axis_size("seq")
    index = lax.axis_index("seq")
    core = lax.axis_index("mp")
    depth = seq.bit_length() - 1
    assert seq == 1 << depth and lax.axis_size("mp") == 2
    values = [(index >> b) & 1 for b in range(depth)]
    top, mate = depth - 1, depth - 2
    lows = list(range(depth - 2))
    orders = (lows, lows[::-1])
    side = values[mate]

    def halves(w):
        half = w.shape[1] // 2
        left, right = w[:, :half], w[:, half:]
        return jnp.where(side == 1, right, left), jnp.where(side == 1, left, right)

    def gather(w):
        keep, give = halves(w)
        pair = join(keep, swap(give, mate, seq), side, 0)
        quad = join(pair, swap(pair, top, seq), values[top], 0)
        cut = cut_point(keep.shape[1])
        parts = (quad[..., :cut], quad[..., cut:])
        return [spread(p, o, (top, mate), values, seq) for p, o in zip(parts, orders)]

    rows, width = encoded.shape
    slots = 2 * seq
    rounds = rows // slots
    counts = frame_tokens[0]
    local = jnp.arange(rows, dtype=jnp.int32)
    ends = jnp.cumsum(counts)
    done = ends[None, :] <= local[:, None]
    frame = index * counts.shape[0] + jnp.sum(done.astype(jnp.int32), axis=1)
    offset = local - jnp.sum(jnp.where(done, counts[None, :], 0), axis=1)
    marks = jnp.stack([frame // 256, frame % 256, offset // 256, offset % 256], axis=1)
    marks = jnp.pad(marks.astype(bf16), ((0, 0), (0, LANE - 4)))
    tiles = width // LANE
    wide = (tiles + 1) // 2 * LANE
    first = encoded[:, :wide]
    second = jnp.concatenate([marks, encoded[:, wide:]], axis=1)
    if second.shape[1] < wide + (LANE if tiles % 2 == 0 else 0):
        raise ValueError("width")
    if tiles % 2 == 0:
        first = jnp.pad(first, ((0, 0), (0, LANE)))
    payload = jnp.where(core == 1, second, first)
    order = jnp.argsort(slot_owner, stable=True).astype(jnp.int32)
    pick = (
        jnp.arange(rounds, dtype=jnp.int32)[None, :, None] * slots + order.reshape(seq, 1, 2)
    ).reshape(-1)
    moved = jnp.take(payload, pick, axis=0).reshape(seq, 2 * rounds, -1)
    arrived = lax.all_to_all(moved, "seq", split_axis=0, concat_axis=0, tiled=True)
    arrived = arrived.reshape(rows, -1)
    both = join(arrived, swap(arrived, mate, seq), side, 0).reshape(2 * rows, -1)
    ready = join(both, swap_core(both), core, 0)
    tokens = jnp.concatenate([ready[0, :, :wide], ready[1, :, LANE:]], axis=1)
    own_marks = lax.dynamic_slice_in_dim(ready[1, :, :4], side * rows, rows, 0).astype(f32)
    frame_ids = own_marks[:, 0] * 256 + own_marks[:, 1]
    offsets = own_marks[:, 2] * 256 + own_marks[:, 3]

    own_b_in, _ = halves(b_in[None, :])
    cut = cut_point(own_b_in.shape[1])
    hidden = []
    for w, b in zip(gather(w_in), (own_b_in[:, :cut], own_b_in[:, cut:])):
        pre = jnp.dot(tokens, w, preferred_element_type=f32) + b.astype(f32)
        part = jax.nn.gelu(pre, approximate=False).astype(bf16)
        hidden.append(part)
    quarter = jnp.concatenate(hidden, axis=1)
    pair_hidden = join(quarter, swap(quarter, mate, seq), side, 0)
    all_hidden = join(pair_hidden, swap_core(pair_hidden), core, 0)
    all_hidden = all_hidden.reshape((4,) + quarter.shape)

    kv = jnp.concatenate([w_key, w_value], axis=1)
    kv_row = join(kv, swap_core(kv), core, 1).reshape(kv.shape[0], -1)
    pairs = [
        (2 * i + h, 2 * (i ^ (1 << top)) + h) for i in range(seq) for h in range(2) if i >> top == h
    ]
    far = lax.ppermute(kv_row, ("seq", "mp"), pairs)
    kv_row = jnp.where(values[top] == core, kv_row, far)
    kv_cut = kv_row.shape[1] // 2
    kv_full = jnp.concatenate(
        [
            spread(p, o, (), values, seq)
            for p, o in zip((kv_row[:, :kv_cut], kv_row[:, kv_cut:]), orders)
        ],
        axis=1,
    )

    own_b_out, _ = halves(b_out[None, :])
    span = own_b_out.shape[1]
    gain = lax.dynamic_slice_in_dim(norm_gain, (2 * core + side) * span, span)[None, :]
    squares = 0.0
    partial = 0.0
    start = 0
    for w in gather(w_out):
        stop = start + w.shape[1]
        blocks = w.reshape(4, -1, w.shape[1])
        summed = own_b_out[:, start:stop].astype(f32)
        for q in range(4):
            summed = summed + jnp.dot(all_hidden[q], blocks[q], preferred_element_type=f32)
        projected = summed.astype(bf16).astype(f32)
        squares = squares + jnp.sum(projected * projected, axis=1)
        scaled = (projected * gain[:, start:stop].astype(f32)).astype(bf16)
        partial = partial + jnp.dot(scaled, kv_full[start:stop], preferred_element_type=f32)
        start = stop

    squares = squares + swap_core(squares)
    squares = squares.reshape(2, rows)
    other_squares = swap(jnp.where(side == 1, squares[0], squares[1]), mate, seq)
    squares = jnp.where(side == 1, squares[1], squares[0]) + other_squares
    inv_rms = lax.rsqrt(squares / norm_gain.shape[0] + norm_eps)[:, None]

    keep = jnp.where(core == 1, partial[:, kv_cut:], partial[:, :kv_cut])
    give = jnp.where(core == 1, partial[:, :kv_cut], partial[:, kv_cut:])
    summed = keep + swap_core(give)
    keep = jnp.where(side == 1, summed[rows:], summed[:rows])
    give = jnp.where(side == 1, summed[:rows], summed[rows:])
    summed = keep + swap(give.astype(bf16), mate, seq).astype(f32)
    linear = summed * inv_rms
    half = w_key.shape[1]
    keys = rotate(linear[:, :half] + b_key.astype(f32), frame_ids, offsets).astype(bf16)
    vals = (linear[:, half:] + b_value.astype(f32)).astype(bf16)
    return keys, vals


ANY = pl.BlockSpec(memory_space=pl.ANY)
VMEM = pl.BlockSpec(memory_space=pltpu.VMEM)
SMEM = pl.BlockSpec(memory_space=pltpu.SMEM)


def place_square(where, pieces, scratch, sems, base=0):
    copies = []
    for d, block in enumerate(pieces):
        parts = block if isinstance(block, tuple) else (block,)
        at = 0
        for part in parts:
            spot = scratch.at[base + (where ^ d)]
            if len(parts) > 1:
                spot = scratch.at[base + (where ^ d), pl.ds(at, part.shape[0])]
            at += part.shape[0]
            copies.append(pltpu.make_async_copy(part, spot, sems.at[len(copies)]))
    return copies


def pick_copy(flag, one, zero, spot, sem):
    @pl.when(flag == 1)
    def _():
        pltpu.make_async_copy(one, spot, sem).start()

    @pl.when(flag == 0)
    def _():
        pltpu.make_async_copy(zero, spot, sem).start()

    return pltpu.make_async_copy(one, spot, sem)


def early_body(spot, mine, other, mine_e, other_e, *refs):
    groups = [list(refs[4 * i : 4 * i + 4]) for i in range(3)]
    out, scratch, hid, sems, hid_sems = refs[12:]
    span = mine.shape[1]
    waits = []
    for i, g in enumerate(groups):
        copies = place_square(spot[0], g, scratch, sems.at[i], 4 * i)
        for c in copies:
            c.start()
        waits += copies
    pairs = ((mine, other), (other, mine), (mine_e, other_e))
    for i, (one, zero) in enumerate(pairs):
        place = hid.at[:, pl.ds(i * span, span)]
        waits.append(pick_copy(spot[1], one, zero, place, hid_sems.at[i]))
    for c in waits:
        c.wait()
    w = scratch[...].reshape(-1, scratch.shape[-1])
    out[...] = jnp.dot(hid[...], w, preferred_element_type=f32)


def early(spot, mine, other, mine_e, other_e, *groups):
    rows = mine.shape[0]
    depth, span = groups[0][0].shape
    return pl.pallas_call(
        early_body,
        out_shape=jax.ShapeDtypeStruct((rows, span), f32),
        in_specs=[SMEM] + [ANY] * 16,
        out_specs=VMEM,
        scratch_shapes=[
            pltpu.VMEM((12, depth, span), bf16),
            pltpu.VMEM((rows, 3 * mine.shape[1]), bf16),
            pltpu.SemaphoreType.DMA((3, 4)),
            pltpu.SemaphoreType.DMA((3,)),
        ],
        name="early",
    )(spot, mine, other, mine_e, other_e, *[p for g in groups for p in g])


def late_body(spot, mine, other, acc, bias, gain, *refs):
    pieces = list(refs[:4])
    scaled, squares, scratch, hid, sems = refs[4:]
    copies = place_square(spot[0], pieces, scratch, sems)
    for c in copies:
        c.start()
    copies.append(pick_copy(spot[1], other, mine, hid, sems.at[4]))
    for c in copies:
        c.wait()
    w = scratch[...].reshape(-1, scratch.shape[-1])
    total = acc[...] + jnp.dot(hid[...], w, preferred_element_type=f32)
    span = total.shape[1]
    b = jnp.where(spot[2] == 1, bias[:, span:], bias[:, :span])
    projected = (total + b.astype(f32)).astype(bf16).astype(f32)
    squares[...] = jnp.sum(projected * projected, axis=1, keepdims=True)
    g = gain[0:1, :].astype(f32)
    for j in range(1, gain.shape[0]):
        g = jnp.where(spot[3] == j, gain[j : j + 1, :].astype(f32), g)
    scaled[...] = (projected * g).astype(bf16)


def late(spot, mine, other, acc, bias, gain, group):
    rows, span = acc.shape
    depth = group[0].shape[0]
    return pl.pallas_call(
        late_body,
        out_shape=[
            jax.ShapeDtypeStruct((rows, span), bf16),
            jax.ShapeDtypeStruct((rows, 1), f32),
        ],
        in_specs=[SMEM, ANY, ANY, VMEM, VMEM, VMEM] + [ANY] * 4,
        out_specs=[VMEM] * 2,
        scratch_shapes=[
            pltpu.VMEM((4, depth, span), bf16),
            pltpu.VMEM(mine.shape, bf16),
            pltpu.SemaphoreType.DMA((5,)),
        ],
        name="late",
    )(spot, mine, other, acc, bias, gain, *group)


def kv_body(spot, scaled, p0, xu, xl, yu, yl, du, dl, keep, give, scratch, sems):
    pieces = [p0, (xu, xl), (yu, yl), (du, dl)]
    copies = place_square(spot[0], pieces, scratch, sems)
    for c in copies:
        c.start()
    for c in copies:
        c.wait()
    w = scratch[...].reshape(-1, scratch.shape[-1])
    total = jnp.dot(scaled[...], w, preferred_element_type=f32)
    half = total.shape[1] // 2

    @pl.when(spot[4] == 0)
    def _():
        keep[...] = total[:, :half]
        give[...] = total[:, half:].astype(bf16)

    @pl.when(spot[4] == 1)
    def _():
        keep[...] = total[:, half:]
        give[...] = total[:, :half].astype(bf16)


def kv_dot(spot, scaled, pieces):
    rows = scaled.shape[0]
    depth, span = pieces[0].shape
    return pl.pallas_call(
        kv_body,
        out_shape=[
            jax.ShapeDtypeStruct((rows, span // 2), f32),
            jax.ShapeDtypeStruct((rows, span // 2), bf16),
        ],
        in_specs=[SMEM, VMEM] + [ANY] * 7,
        out_specs=[VMEM] * 2,
        scratch_shapes=[pltpu.VMEM((4, depth, span), bf16), pltpu.SemaphoreType.DMA((7,))],
        name="kv_dot",
    )(spot, scaled, *pieces)


def shards_square(
    encoded,
    frame_tokens,
    slot_owner,
    w_in,
    b_in,
    w_out,
    b_out,
    norm_gain,
    w_key,
    b_key,
    w_value,
    b_value,
):
    seq = lax.axis_size("seq")
    index = lax.axis_index("seq")
    core = lax.axis_index("mp")
    depth = seq.bit_length() - 1
    top, mate = depth - 1, depth - 2
    side = (index >> mate) & 1
    upper = (index >> top) & 1
    spot = jnp.stack([index & 3, (upper == core).astype(jnp.int32), side, 2 * core + side, core])

    def send(x, *bits):
        flip = sum(1 << b for b in bits)
        return lax.ppermute(x, "seq", [(i, i ^ flip) for i in range(seq)])

    def some(x, pairs):
        return lax.ppermute(x, "seq", pairs)

    def halves(w):
        half = w.shape[1] // 2
        keep = lax.dynamic_slice_in_dim(w, side * half, half, 1)
        return keep, lax.dynamic_slice_in_dim(w, (1 - side) * half, half, 1)

    def square(own, over):
        x = send(own, 0)
        y = send(own, 1)
        return own, x, y, send((y, x)[over], over)

    def ordered(pieces, where, axis):
        low = [jnp.where(where & 1 == 1, pieces[j ^ 1], pieces[j]) for j in range(4)]
        return jnp.stack([jnp.where(where & 2 == 2, low[j ^ 2], low[j]) for j in range(4)], axis)

    in_keep, in_give = halves(w_in)
    out_keep, out_give = halves(w_out)
    in_e = send(in_give, mate)
    in_zk = send(in_keep, top)
    out_own = square(out_keep, 0)
    out_e = send(out_give, mate)
    in_ze = send(in_give, mate, top)
    kv = jnp.concatenate([w_key, w_value], axis=1)
    kv_row = join(kv, swap_core(kv), core, 1).reshape(kv.shape[0], -1)
    out_zk = send(out_keep, top)
    middle = [i for i in range(seq) if (i >> top ^ i >> mate) & 1 == 1]
    both_bits = (1 << top) | (1 << mate)
    near = some(out_give, [(i, i ^ both_bits) for i in middle])
    far_off = some(out_e, [(i, i ^ (1 << top)) for i in middle])
    out_ze = jnp.where(upper != side, near, far_off)
    quad = ordered((in_keep, in_e, in_zk, in_ze), (upper << 1) | side, 0)
    in_pieces = square(quad.reshape(-1, quad.shape[-1]), 1)
    blocks = [p.reshape(quad.shape) for p in in_pieces]
    w_first = ordered(blocks, index & 3, 1).reshape(-1, quad.shape[-1])
    out_from_e = square(out_e, 0)
    out_from_zk = square(out_zk, 1)
    out_from_ze = square(out_ze, 0)
    pairs = [
        (2 * i + h, 2 * (i ^ (1 << top)) + h) for i in range(seq) for h in range(2) if i >> top == h
    ]
    far = lax.ppermute(kv_row, ("seq", "mp"), pairs)
    kv_row = jnp.where(upper == core, kv_row, far)
    mid = kv_row.shape[0] // 2
    kv_u, kv_l = kv_row[:mid], kv_row[mid:]
    kv_xl = send(kv_l, 0)
    kv_yu = send(kv_u, 1)
    kv_xu = send(kv_u, 0)
    kv_yl = send(kv_l, 1)
    kv_du = send(kv_yu, 0)
    kv_dl = send(kv_xl, 1)
    kv_pieces = (kv_row, kv_xu, kv_xl, kv_yu, kv_yl, kv_du, kv_dl)

    rows, width = encoded.shape
    slots = 2 * seq
    rounds = rows // slots
    counts = frame_tokens[0]
    local = jnp.arange(rows, dtype=jnp.int32)
    frame = jnp.full((rows,), index * counts.shape[0], jnp.int32)
    begin = jnp.zeros((rows,), jnp.int32)
    end = 0
    for c in range(counts.shape[0]):
        end = end + counts[c]
        frame = frame + (end <= local).astype(jnp.int32)
        begin = begin + jnp.where(end <= local, counts[c], 0)
    offset = local - begin
    marks = jnp.stack([frame // 256, frame % 256, offset // 256, offset % 256], axis=1)
    marks = jnp.pad(marks.astype(bf16), ((0, 0), (0, LANE - 4)))
    tiles = width // LANE
    wide = (tiles + 1) // 2 * LANE
    first = encoded[:, :wide]
    second = jnp.concatenate([marks, encoded[:, wide:]], axis=1)
    if tiles % 2 == 0:
        first = jnp.pad(first, ((0, 0), (0, LANE)))
    payload = jnp.where(core == 1, second, first)
    slot = jnp.arange(slots, dtype=jnp.int32)
    same = (slot_owner[:, None] == slot_owner[None, :]) & (slot[None, :] < slot[:, None])
    place = slot_owner * (2 * rounds) + jnp.sum(same.astype(jnp.int32), axis=1)
    goal = (place[None, :] + 2 * jnp.arange(rounds, dtype=jnp.int32)[:, None]).reshape(-1)
    select = (local[:, None] == goal[None, :]).astype(bf16)
    moved = jnp.dot(select, payload, preferred_element_type=f32).astype(bf16)
    moved = moved.reshape(seq, 2 * rounds, -1)
    arrived = lax.all_to_all(moved, "seq", split_axis=0, concat_axis=0, tiled=True)
    arrived = arrived.reshape(rows, -1)
    both = join(arrived, send(arrived, mate), side, 0).reshape(2 * rows, -1)
    across = swap_core(both)
    low = jnp.where(core == 1, across, both)
    high = jnp.where(core == 1, both, across)
    tokens = jnp.concatenate([low[:, :wide], high[:, LANE:]], axis=1)
    own_marks = jnp.where(side == 1, high[rows:, :4], high[:rows, :4]).astype(f32)
    frame_ids = own_marks[:, 0] * 256 + own_marks[:, 1]
    offsets = own_marks[:, 2] * 256 + own_marks[:, 3]

    own_b_in, _ = halves(b_in[None, :])
    pre = jnp.dot(tokens, w_first, preferred_element_type=f32) + own_b_in.astype(f32)
    hid = jax.nn.gelu(pre, approximate=False).astype(bf16)
    hid_c = swap_core(hid)
    hid_e = send(hid, mate)
    hid_ce = swap_core(hid_e)

    acc = early(spot, hid, hid_c, hid_e, hid_ce, out_own, out_from_zk, out_from_e)
    gains = norm_gain.reshape(4, -1)
    scaled, squares = late(spot, hid_e, hid_ce, acc, b_out[None, :], gains, out_from_ze)

    squares = squares[:, 0]
    squares = squares + swap_core(squares)
    squares = squares.reshape(2, rows)
    other_squares = send(jnp.where(side == 1, squares[0], squares[1]), mate)
    squares = jnp.where(side == 1, squares[1], squares[0]) + other_squares
    inv_rms = lax.rsqrt(squares / norm_gain.shape[0] + norm_eps)[:, None]

    keep, give = kv_dot(spot, scaled, kv_pieces)
    summed = keep + swap_core(give).astype(f32)
    keep = jnp.where(side == 1, summed[rows:], summed[:rows])
    give = jnp.where(side == 1, summed[:rows], summed[rows:])
    summed = keep + send(give.astype(bf16), mate).astype(f32)
    linear = summed * inv_rms
    half = w_key.shape[1]
    keys = rotate(linear[:, :half] + b_key.astype(f32), frame_ids, offsets).astype(bf16)
    vals = (linear[:, half:] + b_value.astype(f32)).astype(bf16)
    return keys, vals


def solution(mesh):
    square = mesh.shape["seq"] == 16
    return jax.shard_map(
        shards_square if square else shards,
        mesh=mesh,
        in_specs=(
            P("seq", None),
            P("seq", None),
            P(),
            P("seq", "mp"),
            P("mp"),
            P("seq", "mp"),
            P("mp"),
            P(),
            P("seq", "mp"),
            P("mp"),
            P("seq", "mp"),
            P("mp"),
        ),
        out_specs=(P("seq", "mp"), P("seq", "mp")),
        check_vma=False,
    )
```

```python
import jax
import jax.numpy as jnp
from jax import lax
from jax.experimental import pallas as pl
from jax.experimental.pallas import tpu as pltpu
from jax.sharding import PartitionSpec as P

HEAD = 128
TSEC = 16
LANE = 128

norm_eps = 1e-06
rope_base = 1000000.0


f32 = jnp.float32
bf16 = jnp.bfloat16


def rotate(linear, frame_ids, offsets):
    pairs = HEAD // 2
    pair_index = jnp.arange(pairs)
    inverse = jnp.power(f32(rope_base), -2.0 * pair_index.astype(f32) / HEAD)
    chosen = jnp.where(pair_index[None, :] < TSEC, frame_ids[:, None], offsets[:, None])
    angles = chosen * inverse[None, :]
    cosine = jnp.cos(angles)
    sine = jnp.sin(angles)
    turned = []
    for head in range(linear.shape[1] // HEAD):
        first = linear[:, head * HEAD : head * HEAD + pairs]
        second = linear[:, head * HEAD + pairs : (head + 1) * HEAD]
        turned += [first * cosine - second * sine, second * cosine + first * sine]
    return jnp.concatenate(turned, axis=1)


def swap(x, bit, count):
    return lax.ppermute(x, "seq", [(i, i ^ (1 << bit)) for i in range(count)])


def swap_core(x):
    return lax.ppermute(x, "mp", [(0, 1), (1, 0)])


def join(own, other, bit, axis):
    low = jnp.stack([own, other], axis=axis)
    high = jnp.stack([other, own], axis=axis)
    return jnp.where(bit == 1, high, low)


def spread(block, bits, held, values, count):
    held = list(held)
    for bit in bits:
        other = swap(block, bit, count)
        axis = sum(1 for b in held if b > bit)
        block = join(block, other, values[bit], axis)
        held.insert(axis, bit)
    return block.reshape(-1, block.shape[-1])


def cut_point(width):
    return (width // LANE + 1) // 2 * LANE


def shards(
    encoded,
    frame_tokens,
    slot_owner,
    w_in,
    b_in,
    w_out,
    b_out,
    norm_gain,
    w_key,
    b_key,
    w_value,
    b_value,
):
    seq = lax.axis_size("seq")
    index = lax.axis_index("seq")
    core = lax.axis_index("mp")
    depth = seq.bit_length() - 1
    assert seq == 1 << depth and lax.axis_size("mp") == 2
    values = [(index >> b) & 1 for b in range(depth)]
    top, mate = depth - 1, depth - 2
    lows = list(range(depth - 2))
    orders = (lows, lows[::-1])
    side = values[mate]

    def halves(w):
        half = w.shape[1] // 2
        left, right = w[:, :half], w[:, half:]
        return jnp.where(side == 1, right, left), jnp.where(side == 1, left, right)

    def gather(w):
        keep, give = halves(w)
        pair = join(keep, swap(give, mate, seq), side, 0)
        quad = join(pair, swap(pair, top, seq), values[top], 0)
        cut = cut_point(keep.shape[1])
        parts = (quad[..., :cut], quad[..., cut:])
        return [spread(p, o, (top, mate), values, seq) for p, o in zip(parts, orders)]

    rows, width = encoded.shape
    slots = 2 * seq
    rounds = rows // slots
    counts = frame_tokens[0]
    local = jnp.arange(rows, dtype=jnp.int32)
    ends = jnp.cumsum(counts)
    done = ends[None, :] <= local[:, None]
    frame = index * counts.shape[0] + jnp.sum(done.astype(jnp.int32), axis=1)
    offset = local - jnp.sum(jnp.where(done, counts[None, :], 0), axis=1)
    marks = jnp.stack([frame // 256, frame % 256, offset // 256, offset % 256], axis=1)
    marks = jnp.pad(marks.astype(bf16), ((0, 0), (0, LANE - 4)))
    tiles = width // LANE
    wide = (tiles + 1) // 2 * LANE
    first = encoded[:, :wide]
    second = jnp.concatenate([marks, encoded[:, wide:]], axis=1)
    if second.shape[1] < wide + (LANE if tiles % 2 == 0 else 0):
        raise ValueError("width")
    if tiles % 2 == 0:
        first = jnp.pad(first, ((0, 0), (0, LANE)))
    payload = jnp.where(core == 1, second, first)
    order = jnp.argsort(slot_owner, stable=True).astype(jnp.int32)
    pick = (
        jnp.arange(rounds, dtype=jnp.int32)[None, :, None] * slots + order.reshape(seq, 1, 2)
    ).reshape(-1)
    moved = jnp.take(payload, pick, axis=0).reshape(seq, 2 * rounds, -1)
    arrived = lax.all_to_all(moved, "seq", split_axis=0, concat_axis=0, tiled=True)
    arrived = arrived.reshape(rows, -1)
    both = join(arrived, swap(arrived, mate, seq), side, 0).reshape(2 * rows, -1)
    ready = join(both, swap_core(both), core, 0)
    tokens = jnp.concatenate([ready[0, :, :wide], ready[1, :, LANE:]], axis=1)
    own_marks = lax.dynamic_slice_in_dim(ready[1, :, :4], side * rows, rows, 0).astype(f32)
    frame_ids = own_marks[:, 0] * 256 + own_marks[:, 1]
    offsets = own_marks[:, 2] * 256 + own_marks[:, 3]

    own_b_in, _ = halves(b_in[None, :])
    cut = cut_point(own_b_in.shape[1])
    hidden = []
    for w, b in zip(gather(w_in), (own_b_in[:, :cut], own_b_in[:, cut:])):
        pre = jnp.dot(tokens, w, preferred_element_type=f32) + b.astype(f32)
        part = jax.nn.gelu(pre, approximate=False).astype(bf16)
        hidden.append(part)
    quarter = jnp.concatenate(hidden, axis=1)
    pair_hidden = join(quarter, swap(quarter, mate, seq), side, 0)
    all_hidden = join(pair_hidden, swap_core(pair_hidden), core, 0)
    all_hidden = all_hidden.reshape((4,) + quarter.shape)

    kv = jnp.concatenate([w_key, w_value], axis=1)
    kv_row = join(kv, swap_core(kv), core, 1).reshape(kv.shape[0], -1)
    pairs = [
        (2 * i + h, 2 * (i ^ (1 << top)) + h) for i in range(seq) for h in range(2) if i >> top == h
    ]
    far = lax.ppermute(kv_row, ("seq", "mp"), pairs)
    kv_row = jnp.where(values[top] == core, kv_row, far)
    kv_cut = kv_row.shape[1] // 2
    kv_full = jnp.concatenate(
        [
            spread(p, o, (), values, seq)
            for p, o in zip((kv_row[:, :kv_cut], kv_row[:, kv_cut:]), orders)
        ],
        axis=1,
    )

    own_b_out, _ = halves(b_out[None, :])
    span = own_b_out.shape[1]
    gain = lax.dynamic_slice_in_dim(norm_gain, (2 * core + side) * span, span)[None, :]
    squares = 0.0
    partial = 0.0
    start = 0
    for w in gather(w_out):
        stop = start + w.shape[1]
        blocks = w.reshape(4, -1, w.shape[1])
        summed = own_b_out[:, start:stop].astype(f32)
        for q in range(4):
            summed = summed + jnp.dot(all_hidden[q], blocks[q], preferred_element_type=f32)
        projected = summed.astype(bf16).astype(f32)
        squares = squares + jnp.sum(projected * projected, axis=1)
        scaled = (projected * gain[:, start:stop].astype(f32)).astype(bf16)
        partial = partial + jnp.dot(scaled, kv_full[start:stop], preferred_element_type=f32)
        start = stop

    squares = squares + swap_core(squares)
    squares = squares.reshape(2, rows)
    other_squares = swap(jnp.where(side == 1, squares[0], squares[1]), mate, seq)
    squares = jnp.where(side == 1, squares[1], squares[0]) + other_squares
    inv_rms = lax.rsqrt(squares / norm_gain.shape[0] + norm_eps)[:, None]

    keep = jnp.where(core == 1, partial[:, kv_cut:], partial[:, :kv_cut])
    give = jnp.where(core == 1, partial[:, :kv_cut], partial[:, kv_cut:])
    summed = keep + swap_core(give)
    keep = jnp.where(side == 1, summed[rows:], summed[:rows])
    give = jnp.where(side == 1, summed[:rows], summed[rows:])
    summed = keep + swap(give.astype(bf16), mate, seq).astype(f32)
    linear = summed * inv_rms
    half = w_key.shape[1]
    keys = rotate(linear[:, :half] + b_key.astype(f32), frame_ids, offsets).astype(bf16)
    vals = (linear[:, half:] + b_value.astype(f32)).astype(bf16)
    return keys, vals


ANY = pl.BlockSpec(memory_space=pl.ANY)
VMEM = pl.BlockSpec(memory_space=pltpu.VMEM)
SMEM = pl.BlockSpec(memory_space=pltpu.SMEM)


def place_square(where, pieces, scratch, sems, base=0):
    copies = []
    for d, block in enumerate(pieces):
        parts = block if isinstance(block, tuple) else (block,)
        at = 0
        for part in parts:
            spot = scratch.at[base + (where ^ d)]
            if len(parts) > 1:
                spot = scratch.at[base + (where ^ d), pl.ds(at, part.shape[0])]
            at += part.shape[0]
            copies.append(pltpu.make_async_copy(part, spot, sems.at[len(copies)]))
    return copies


def pick_copy(flag, one, zero, spot, sem):
    @pl.when(flag == 1)
    def _():
        pltpu.make_async_copy(one, spot, sem).start()

    @pl.when(flag == 0)
    def _():
        pltpu.make_async_copy(zero, spot, sem).start()

    return pltpu.make_async_copy(one, spot, sem)


def first_body(spot, *refs):
    mine, other, mate, mate_other = refs[:4]
    quads = refs[4:8]
    bias = refs[8]
    out, tokens, w, sems, tok_sems = refs[-5:]
    rows, wide = mine.shape
    rest = tokens.shape[1] - wide
    waits = []
    for d, quad in enumerate(quads):
        for z in range(4):
            place = w.at[(spot[5] ^ z) * 4 + (spot[0] ^ d)]
            waits.append(pltpu.make_async_copy(quad.at[z], place, sems.at[d, z]))
    for c in waits:
        c.start()
    skip = wide - rest
    for i, (one, zero) in enumerate(((mine, other), (mate, mate_other))):
        at = pl.ds(pl.multiple_of((spot[2] ^ i) * rows, rows), rows)
        low, high = tokens.at[at, pl.ds(0, wide)], tokens.at[at, pl.ds(wide, rest)]
        cut = pl.ds(skip, rest)
        waits.append(pick_copy(spot[4], zero, one, low, tok_sems.at[i, 0]))
        waits.append(
            pick_copy(spot[4], one.at[:, cut], zero.at[:, cut], high, tok_sems.at[i, 1])
        )
    for c in waits:
        c.wait()
    weights = w[...].reshape(-1, w.shape[-1])
    span = weights.shape[1]
    b = jnp.where(spot[2] == 1, bias[:, span:], bias[:, :span]).astype(f32)
    part = rows // 2
    for i in range(4):
        at = slice(i * part, (i + 1) * part)
        pre = jnp.dot(tokens[at, :], weights, preferred_element_type=f32) + b
        out[at, :] = (0.5 * pre * (1.0 + lax.erf(pre * (0.5**0.5)))).astype(bf16)


def first(spot, own, quads, bias, width, *unused):
    rows, _ = own[0].shape
    span = quads[0].shape[-1]
    return pl.pallas_call(
        first_body,
        out_shape=jax.ShapeDtypeStruct((2 * rows, span), bf16),
        in_specs=[SMEM] + [ANY] * 8 + [VMEM] + [ANY] * len(unused),
        out_specs=VMEM,
        scratch_shapes=[
            pltpu.VMEM((2 * rows, width), bf16),
            pltpu.VMEM((16,) + quads[0].shape[1:], bf16),
            pltpu.SemaphoreType.DMA((4, 4)),
            pltpu.SemaphoreType.DMA((2, 2)),
        ],
        name="first",
    )(spot, *own, *quads, bias, *unused)


def early_body(spot, mine, other, *refs):
    groups = [list(refs[4 * i : 4 * i + 4]) for i in range(2)]
    out, scratch, hid, sems, hid_sems = refs[8:]
    waits = []
    for i, (one, zero) in enumerate(((mine, other), (other, mine))):
        copies = [pick_copy(spot[1], one, zero, hid.at[i], hid_sems.at[i])]
        pieces = place_square(spot[0], groups[i], scratch, sems.at[i], 4 * i)
        for c in pieces:
            c.start()
        waits.append(copies + pieces)
    for i in range(2):
        for c in waits[i]:
            c.wait()
        w = scratch[4 * i : 4 * i + 4].reshape(-1, scratch.shape[-1])
        part = jnp.dot(hid[i], w, preferred_element_type=f32)
        if i == 0:
            out[...] = part
        else:
            out[...] += part


def early(spot, mine, other, *groups):
    rows = mine.shape[0]
    depth, span = groups[0][0].shape
    return pl.pallas_call(
        early_body,
        out_shape=jax.ShapeDtypeStruct((rows, span), f32),
        in_specs=[SMEM] + [ANY] * 10,
        out_specs=VMEM,
        scratch_shapes=[
            pltpu.VMEM((8, depth, span), bf16),
            pltpu.VMEM((2,) + mine.shape, bf16),
            pltpu.SemaphoreType.DMA((2, 4)),
            pltpu.SemaphoreType.DMA((2,)),
        ],
        name="early",
    )(spot, mine, other, *[p for g in groups for p in g])


def final_body(spot, mine, other, acc, bias, gain, *refs):
    groups = [list(refs[:4]), list(refs[4:8])]
    p0, xu, xl, yu, yl, du, dl = refs[8:15]
    own_keep, oth_keep, give, squares = refs[15:19]
    scratch, hid, base, kv, sems, hid_sems, kv_sems = refs[19:]
    waits = []
    for i, (one, zero) in enumerate(((mine, other), (other, mine))):
        copies = [pick_copy(spot[1], one, zero, hid.at[i], hid_sems.at[i])]
        pieces = place_square(spot[0], groups[i], scratch, sems.at[i], 4 * i)
        for c in pieces:
            c.start()
        waits.append(copies + pieces)
    load = pltpu.make_async_copy(acc, base, hid_sems.at[2])
    load.start()
    waits[1].append(load)
    kv_copies = place_square(spot[0], [p0, (xu, xl), (yu, yl), (du, dl)], kv, kv_sems)
    for c in kv_copies:
        c.start()
    span = base.shape[1]
    b = jnp.where(spot[2] == 1, bias[:, span:], bias[:, :span]).astype(f32)
    g = gain[0:1, :].astype(f32)
    for j in range(1, gain.shape[0]):
        g = jnp.where(spot[3] == j, gain[j : j + 1, :].astype(f32), g)
    for c in waits[0]:
        c.wait()
    w = scratch[0:4].reshape(-1, span)
    before = jnp.dot(hid[0], w, preferred_element_type=f32)
    for c in waits[1]:
        c.wait()
    base[...] += before
    for c in kv_copies:
        c.wait()
    rows = own_keep.shape[0]
    half = own_keep.shape[1]
    w = scratch[4:8].reshape(-1, span)
    kv_rows = kv[...].reshape(-1, kv.shape[-1])
    part = rows // 2
    for i in range(4):
        at = slice(i * part, (i + 1) * part)
        total = base[at, :] + jnp.dot(hid[1, at, :], w, preferred_element_type=f32)
        projected = (total + b).astype(bf16).astype(f32)
        squares[at, :] = jnp.sum(projected * projected, axis=1, keepdims=True)
        scaled = (projected * g).astype(bf16)
        got = jnp.dot(scaled, kv_rows, preferred_element_type=f32)
        left, right = got[:, :half], got[:, half:]
        keep = jnp.where(spot[4] == 1, right, left)
        base[at, :half] = keep
        slot = jnp.where(spot[2] == i // 2, rows, 0)
        place = pl.ds(pl.multiple_of(slot + (i % 2) * part, part), part)
        give[place, :] = jnp.where(spot[4] == 1, left, right).astype(bf16)

    @pl.when(spot[2] == 0)
    def _():
        own_keep[...] = base[:rows, :half]
        oth_keep[...] = base[rows:, :half]

    @pl.when(spot[2] == 1)
    def _():
        own_keep[...] = base[rows:, :half]
        oth_keep[...] = base[:rows, :half]


def final(spot, mine, other, acc, bias, gain, groups, kv_pieces):
    rows, span = acc.shape
    depth = groups[0][0].shape[0]
    kv_depth, width = kv_pieces[0].shape
    keep = jax.ShapeDtypeStruct((rows // 2, width // 2), f32)
    return pl.pallas_call(
        final_body,
        out_shape=[
            keep,
            keep,
            jax.ShapeDtypeStruct((rows, width // 2), bf16),
            jax.ShapeDtypeStruct((rows, 1), f32),
        ],
        in_specs=[SMEM, ANY, ANY, ANY, VMEM, VMEM] + [ANY] * 15,
        out_specs=[VMEM] * 4,
        scratch_shapes=[
            pltpu.VMEM((8, depth, span), bf16),
            pltpu.VMEM((2,) + mine.shape, bf16),
            pltpu.VMEM((rows, span), f32),
            pltpu.VMEM((4, kv_depth, width), bf16),
            pltpu.SemaphoreType.DMA((2, 4)),
            pltpu.SemaphoreType.DMA((3,)),
            pltpu.SemaphoreType.DMA((7,)),
        ],
        name="final",
    )(spot, mine, other, acc, bias, gain, *groups[0], *groups[1], *kv_pieces)


def shards_square(
    encoded,
    frame_tokens,
    slot_owner,
    w_in,
    b_in,
    w_out,
    b_out,
    norm_gain,
    w_key,
    b_key,
    w_value,
    b_value,
):
    seq = lax.axis_size("seq")
    index = lax.axis_index("seq")
    core = lax.axis_index("mp")
    depth = seq.bit_length() - 1
    top, mate = depth - 1, depth - 2
    side = (index >> mate) & 1
    upper = (index >> top) & 1
    spot = jnp.stack(
        [index & 3, (upper == core).astype(jnp.int32), side, 2 * core + side, core, 2 * upper + side]
    )

    def send(x, *bits):
        flip = sum(1 << b for b in bits)
        return lax.ppermute(x, "seq", [(i, i ^ flip) for i in range(seq)])

    def some(x, pairs):
        return lax.ppermute(x, "seq", pairs)

    def halves(w):
        half = w.shape[1] // 2
        keep = lax.dynamic_slice_in_dim(w, side * half, half, 1)
        return keep, lax.dynamic_slice_in_dim(w, (1 - side) * half, half, 1)

    def square(own, over):
        x = send(own, 0)
        y = send(own, 1)
        return own, x, y, send((y, x)[over], over)

    in_keep, in_give = halves(w_in)
    out_keep, out_give = halves(w_out)
    in_e = send(in_give, mate)
    in_zk = send(in_keep, top)
    out_own = square(out_keep, 0)
    out_e = send(out_give, mate)
    in_ze = send(in_give, mate, top)
    kv = jnp.concatenate([w_key, w_value], axis=1)
    kv_row = join(kv, swap_core(kv), core, 1).reshape(kv.shape[0], -1)
    out_zk = send(out_keep, top)
    middle = [i for i in range(seq) if (i >> top ^ i >> mate) & 1 == 1]
    both_bits = (1 << top) | (1 << mate)
    near = some(out_give, [(i, i ^ both_bits) for i in middle])
    far_off = some(out_e, [(i, i ^ (1 << top)) for i in middle])
    out_ze = jnp.where(upper != side, near, far_off)
    quad = jnp.concatenate([in_keep, in_e, in_zk, in_ze])
    in_pieces = square(quad, 1)
    in_quads = [p.reshape((4,) + in_keep.shape) for p in in_pieces]
    out_from_e = square(out_e, 0)
    out_from_zk = square(out_zk, 1)
    out_from_ze = square(out_ze, 0)
    pairs = [
        (2 * i + h, 2 * (i ^ (1 << top)) + h) for i in range(seq) for h in range(2) if i >> top == h
    ]
    far = lax.ppermute(kv_row, ("seq", "mp"), pairs)
    kv_row = jnp.where(upper == core, kv_row, far)
    mid = kv_row.shape[0] // 2
    kv_u, kv_l = kv_row[:mid], kv_row[mid:]
    kv_xl = send(kv_l, 0)
    kv_yu = send(kv_u, 1)
    kv_xu = send(kv_u, 0)
    kv_yl = send(kv_l, 1)
    kv_du = send(kv_xu, 1)
    kv_dl = send(kv_xl, 1)
    kv_pieces = (kv_row, kv_xu, kv_xl, kv_yu, kv_yl, kv_du, kv_dl)

    rows, width = encoded.shape
    slots = 2 * seq
    rounds = rows // slots
    counts = frame_tokens[0]
    local = jnp.arange(rows, dtype=jnp.int32)
    frame = jnp.full((rows,), index * counts.shape[0], jnp.int32)
    begin = jnp.zeros((rows,), jnp.int32)
    end = 0
    for c in range(counts.shape[0]):
        end = end + counts[c]
        frame = frame + (end <= local).astype(jnp.int32)
        begin = begin + jnp.where(end <= local, counts[c], 0)
    offset = local - begin
    marks = jnp.stack([frame // 256, frame % 256, offset // 256, offset % 256], axis=1)
    marks = jnp.pad(marks.astype(bf16), ((0, 0), (0, LANE - 4)))
    tiles = width // LANE
    wide = (tiles + 1) // 2 * LANE
    low_half = encoded[:, :wide]
    second = jnp.concatenate([marks, encoded[:, wide:]], axis=1)
    if tiles % 2 == 0:
        low_half = jnp.pad(low_half, ((0, 0), (0, LANE)))
    payload = jnp.where(core == 1, second, low_half)
    slot = jnp.arange(slots, dtype=jnp.int32)
    same = (slot_owner[:, None] == slot_owner[None, :]) & (slot[None, :] < slot[:, None])
    place = slot_owner * (2 * rounds) + jnp.sum(same.astype(jnp.int32), axis=1)
    goal = (place[None, :] + 2 * jnp.arange(rounds, dtype=jnp.int32)[:, None]).reshape(-1)
    select = (local[:, None] == goal[None, :]).astype(bf16)
    moved = jnp.dot(select, payload, preferred_element_type=f32).astype(bf16)
    moved = moved.reshape(seq, 2 * rounds, -1)
    arrived = lax.all_to_all(moved, "seq", split_axis=0, concat_axis=0, tiled=True)
    arrived = arrived.reshape(rows, -1)
    other = swap_core(arrived)
    mate_rows = send(arrived, mate)
    own_tokens = (arrived, other, mate_rows, swap_core(mate_rows))
    own_marks = jnp.where(core == 1, arrived[:, :4], other[:, :4]).astype(f32)
    frame_ids = own_marks[:, 0] * 256 + own_marks[:, 1]
    offsets = own_marks[:, 2] * 256 + own_marks[:, 3]

    bias, gains = b_out[None, :], norm_gain.reshape(4, -1)
    hid = first(spot, own_tokens, in_quads, b_in[None, :], width, bias, gains)
    hid_c = swap_core(hid)
    hid_e = send(hid, mate)
    hid_ce = swap_core(hid_e)

    acc = early(spot, hid, hid_c, out_own, out_from_zk)
    own_keep, oth_keep, give, squares = final(
        spot, hid_e, hid_ce, acc, bias, gains, (out_from_e, out_from_ze), kv_pieces
    )

    crossed = swap_core(give)
    oth_sum = (oth_keep + crossed[:rows].astype(f32)).astype(bf16)
    mate_sum = send(oth_sum, mate)
    squares = squares[:, 0]
    squares = squares + swap_core(squares)
    squares = squares.reshape(2, rows)
    other_squares = send(jnp.where(side == 1, squares[0], squares[1]), mate)
    squares = jnp.where(side == 1, squares[1], squares[0]) + other_squares
    inv_rms = lax.rsqrt(squares / norm_gain.shape[0] + norm_eps)[:, None]
    summed = own_keep + crossed[rows:].astype(f32) + mate_sum.astype(f32)
    linear = summed * inv_rms
    half = w_key.shape[1]
    keys = rotate(linear[:, :half] + b_key.astype(f32), frame_ids, offsets).astype(bf16)
    vals = (linear[:, half:] + b_value.astype(f32)).astype(bf16)
    return keys, vals


def solution(mesh):
    square = mesh.shape["seq"] == 16
    return jax.shard_map(
        shards_square if square else shards,
        mesh=mesh,
        in_specs=(
            P("seq", None),
            P("seq", None),
            P(),
            P("seq", "mp"),
            P("mp"),
            P("seq", "mp"),
            P("mp"),
            P(),
            P("seq", "mp"),
            P("mp"),
            P("seq", "mp"),
            P("mp"),
        ),
        out_specs=(P("seq", "mp"), P("seq", "mp")),
        check_vma=False,
    )
```

```python
import jax
import jax.numpy as jnp
from jax import lax
from jax.experimental import pallas as pl
from jax.experimental.pallas import tpu as pltpu
from jax.sharding import PartitionSpec as P

HEAD = 128
TSEC = 16
LANE = 128

norm_eps = 1e-06
rope_base = 1000000.0


f32 = jnp.float32
bf16 = jnp.bfloat16


def rotate(linear, frame_ids, offsets):
    pairs = HEAD // 2
    pair_index = jnp.arange(pairs)
    inverse = jnp.power(f32(rope_base), -2.0 * pair_index.astype(f32) / HEAD)
    chosen = jnp.where(pair_index[None, :] < TSEC, frame_ids[:, None], offsets[:, None])
    angles = chosen * inverse[None, :]
    cosine = jnp.cos(angles)
    sine = jnp.sin(angles)
    turned = []
    for head in range(linear.shape[1] // HEAD):
        first = linear[:, head * HEAD : head * HEAD + pairs]
        second = linear[:, head * HEAD + pairs : (head + 1) * HEAD]
        turned += [first * cosine - second * sine, second * cosine + first * sine]
    return jnp.concatenate(turned, axis=1)


def swap(x, bit, count):
    return lax.ppermute(x, "seq", [(i, i ^ (1 << bit)) for i in range(count)])


def swap_core(x):
    return lax.ppermute(x, "mp", [(0, 1), (1, 0)])


def join(own, other, bit, axis):
    low = jnp.stack([own, other], axis=axis)
    high = jnp.stack([other, own], axis=axis)
    return jnp.where(bit == 1, high, low)


def spread(block, bits, held, values, count):
    held = list(held)
    for bit in bits:
        other = swap(block, bit, count)
        axis = sum(1 for b in held if b > bit)
        block = join(block, other, values[bit], axis)
        held.insert(axis, bit)
    return block.reshape(-1, block.shape[-1])


def cut_point(width):
    return (width // LANE + 1) // 2 * LANE


def shards(
    encoded,
    frame_tokens,
    slot_owner,
    w_in,
    b_in,
    w_out,
    b_out,
    norm_gain,
    w_key,
    b_key,
    w_value,
    b_value,
):
    seq = lax.axis_size("seq")
    index = lax.axis_index("seq")
    core = lax.axis_index("mp")
    depth = seq.bit_length() - 1
    assert seq == 1 << depth and lax.axis_size("mp") == 2
    values = [(index >> b) & 1 for b in range(depth)]
    top, mate = depth - 1, depth - 2
    lows = list(range(depth - 2))
    orders = (lows, lows[::-1])
    side = values[mate]

    def halves(w):
        half = w.shape[1] // 2
        left, right = w[:, :half], w[:, half:]
        return jnp.where(side == 1, right, left), jnp.where(side == 1, left, right)

    def gather(w):
        keep, give = halves(w)
        pair = join(keep, swap(give, mate, seq), side, 0)
        quad = join(pair, swap(pair, top, seq), values[top], 0)
        cut = cut_point(keep.shape[1])
        parts = (quad[..., :cut], quad[..., cut:])
        return [spread(p, o, (top, mate), values, seq) for p, o in zip(parts, orders)]

    rows, width = encoded.shape
    slots = 2 * seq
    rounds = rows // slots
    counts = frame_tokens[0]
    local = jnp.arange(rows, dtype=jnp.int32)
    ends = jnp.cumsum(counts)
    done = ends[None, :] <= local[:, None]
    frame = index * counts.shape[0] + jnp.sum(done.astype(jnp.int32), axis=1)
    offset = local - jnp.sum(jnp.where(done, counts[None, :], 0), axis=1)
    marks = jnp.stack([frame // 256, frame % 256, offset // 256, offset % 256], axis=1)
    marks = jnp.pad(marks.astype(bf16), ((0, 0), (0, LANE - 4)))
    tiles = width // LANE
    wide = (tiles + 1) // 2 * LANE
    first = encoded[:, :wide]
    second = jnp.concatenate([marks, encoded[:, wide:]], axis=1)
    if second.shape[1] < wide + (LANE if tiles % 2 == 0 else 0):
        raise ValueError("width")
    if tiles % 2 == 0:
        first = jnp.pad(first, ((0, 0), (0, LANE)))
    payload = jnp.where(core == 1, second, first)
    order = jnp.argsort(slot_owner, stable=True).astype(jnp.int32)
    pick = (
        jnp.arange(rounds, dtype=jnp.int32)[None, :, None] * slots + order.reshape(seq, 1, 2)
    ).reshape(-1)
    moved = jnp.take(payload, pick, axis=0).reshape(seq, 2 * rounds, -1)
    arrived = lax.all_to_all(moved, "seq", split_axis=0, concat_axis=0, tiled=True)
    arrived = arrived.reshape(rows, -1)
    both = join(arrived, swap(arrived, mate, seq), side, 0).reshape(2 * rows, -1)
    ready = join(both, swap_core(both), core, 0)
    tokens = jnp.concatenate([ready[0, :, :wide], ready[1, :, LANE:]], axis=1)
    own_marks = lax.dynamic_slice_in_dim(ready[1, :, :4], side * rows, rows, 0).astype(f32)
    frame_ids = own_marks[:, 0] * 256 + own_marks[:, 1]
    offsets = own_marks[:, 2] * 256 + own_marks[:, 3]

    own_b_in, _ = halves(b_in[None, :])
    cut = cut_point(own_b_in.shape[1])
    hidden = []
    for w, b in zip(gather(w_in), (own_b_in[:, :cut], own_b_in[:, cut:])):
        pre = jnp.dot(tokens, w, preferred_element_type=f32) + b.astype(f32)
        part = jax.nn.gelu(pre, approximate=False).astype(bf16)
        hidden.append(part)
    quarter = jnp.concatenate(hidden, axis=1)
    pair_hidden = join(quarter, swap(quarter, mate, seq), side, 0)
    all_hidden = join(pair_hidden, swap_core(pair_hidden), core, 0)
    all_hidden = all_hidden.reshape((4,) + quarter.shape)

    kv = jnp.concatenate([w_key, w_value], axis=1)
    kv_row = join(kv, swap_core(kv), core, 1).reshape(kv.shape[0], -1)
    pairs = [
        (2 * i + h, 2 * (i ^ (1 << top)) + h) for i in range(seq) for h in range(2) if i >> top == h
    ]
    far = lax.ppermute(kv_row, ("seq", "mp"), pairs)
    kv_row = jnp.where(values[top] == core, kv_row, far)
    kv_cut = kv_row.shape[1] // 2
    kv_full = jnp.concatenate(
        [
            spread(p, o, (), values, seq)
            for p, o in zip((kv_row[:, :kv_cut], kv_row[:, kv_cut:]), orders)
        ],
        axis=1,
    )

    own_b_out, _ = halves(b_out[None, :])
    span = own_b_out.shape[1]
    gain = lax.dynamic_slice_in_dim(norm_gain, (2 * core + side) * span, span)[None, :]
    squares = 0.0
    partial = 0.0
    start = 0
    for w in gather(w_out):
        stop = start + w.shape[1]
        blocks = w.reshape(4, -1, w.shape[1])
        summed = own_b_out[:, start:stop].astype(f32)
        for q in range(4):
            summed = summed + jnp.dot(all_hidden[q], blocks[q], preferred_element_type=f32)
        projected = summed.astype(bf16).astype(f32)
        squares = squares + jnp.sum(projected * projected, axis=1)
        scaled = (projected * gain[:, start:stop].astype(f32)).astype(bf16)
        partial = partial + jnp.dot(scaled, kv_full[start:stop], preferred_element_type=f32)
        start = stop

    squares = squares + swap_core(squares)
    squares = squares.reshape(2, rows)
    other_squares = swap(jnp.where(side == 1, squares[0], squares[1]), mate, seq)
    squares = jnp.where(side == 1, squares[1], squares[0]) + other_squares
    inv_rms = lax.rsqrt(squares / norm_gain.shape[0] + norm_eps)[:, None]

    keep = jnp.where(core == 1, partial[:, kv_cut:], partial[:, :kv_cut])
    give = jnp.where(core == 1, partial[:, :kv_cut], partial[:, kv_cut:])
    summed = keep + swap_core(give)
    keep = jnp.where(side == 1, summed[rows:], summed[:rows])
    give = jnp.where(side == 1, summed[:rows], summed[rows:])
    summed = keep + swap(give.astype(bf16), mate, seq).astype(f32)
    linear = summed * inv_rms
    half = w_key.shape[1]
    keys = rotate(linear[:, :half] + b_key.astype(f32), frame_ids, offsets).astype(bf16)
    vals = (linear[:, half:] + b_value.astype(f32)).astype(bf16)
    return keys, vals


ANY = pl.BlockSpec(memory_space=pl.ANY)
VMEM = pl.BlockSpec(memory_space=pltpu.VMEM)
SMEM = pl.BlockSpec(memory_space=pltpu.SMEM)


def place_square(where, pieces, scratch, sems, base=0):
    copies = []
    for d, block in enumerate(pieces):
        parts = block if isinstance(block, tuple) else (block,)
        at = 0
        for part in parts:
            spot = scratch.at[base + (where ^ d)]
            if len(parts) > 1:
                spot = scratch.at[base + (where ^ d), pl.ds(at, part.shape[0])]
            at += part.shape[0]
            copies.append(pltpu.make_async_copy(part, spot, sems.at[len(copies)]))
    return copies


def pick_copy(flag, one, zero, spot, sem):
    @pl.when(flag == 1)
    def _():
        pltpu.make_async_copy(one, spot, sem).start()

    @pl.when(flag == 0)
    def _():
        pltpu.make_async_copy(zero, spot, sem).start()

    return pltpu.make_async_copy(one, spot, sem)


def first_body(spot, *refs):
    mine, other, mate, mate_other = refs[:4]
    quads = refs[4:8]
    bias = refs[8]
    out, tokens, w, sems, tok_sems = refs[-5:]
    rows, wide = mine.shape
    rest = tokens.shape[1] - wide
    waits = []
    for d, quad in enumerate(quads):
        for z in range(4):
            place = w.at[(spot[5] ^ z) * 4 + (spot[0] ^ d)]
            waits.append(pltpu.make_async_copy(quad.at[z], place, sems.at[d, z]))
    for c in waits:
        c.start()
    skip = wide - rest
    for i, (one, zero) in enumerate(((mine, other), (mate, mate_other))):
        at = pl.ds(pl.multiple_of((spot[2] ^ i) * rows, rows), rows)
        low, high = tokens.at[at, pl.ds(0, wide)], tokens.at[at, pl.ds(wide, rest)]
        cut = pl.ds(skip, rest)
        waits.append(pick_copy(spot[4], zero, one, low, tok_sems.at[i, 0]))
        waits.append(
            pick_copy(spot[4], one.at[:, cut], zero.at[:, cut], high, tok_sems.at[i, 1])
        )
    for c in waits:
        c.wait()
    weights = w[...].reshape(-1, w.shape[-1])
    span = weights.shape[1]
    b = jnp.where(spot[2] == 1, bias[:, span:], bias[:, :span]).astype(f32)
    part = rows // 2
    for i in range(4):
        at = slice(i * part, (i + 1) * part)
        pre = jnp.dot(tokens[at, :], weights, preferred_element_type=f32) + b
        out[at, :] = (0.5 * pre * (1.0 + lax.erf(pre * (0.5**0.5)))).astype(bf16)


def first(spot, own, quads, bias, width, *unused):
    rows, _ = own[0].shape
    span = quads[0].shape[-1]
    return pl.pallas_call(
        first_body,
        out_shape=jax.ShapeDtypeStruct((2 * rows, span), bf16),
        in_specs=[SMEM] + [ANY] * 8 + [VMEM] + [ANY] * len(unused),
        out_specs=VMEM,
        scratch_shapes=[
            pltpu.VMEM((2 * rows, width), bf16),
            pltpu.VMEM((16,) + quads[0].shape[1:], bf16),
            pltpu.SemaphoreType.DMA((4, 4)),
            pltpu.SemaphoreType.DMA((2, 2)),
        ],
        name="first",
    )(spot, *own, *quads, bias, *unused)


def early_body(spot, mine, other, *refs):
    groups = [list(refs[4 * i : 4 * i + 4]) for i in range(2)]
    out, scratch, hid, sems, hid_sems = refs[8:]
    waits = []
    for i, (one, zero) in enumerate(((mine, other), (other, mine))):
        copies = [pick_copy(spot[1], one, zero, hid.at[i], hid_sems.at[i])]
        pieces = place_square(spot[0], groups[i], scratch, sems.at[i], 4 * i)
        for c in pieces:
            c.start()
        waits.append(copies + pieces)
    for i in range(2):
        for c in waits[i]:
            c.wait()
        w = scratch[4 * i : 4 * i + 4].reshape(-1, scratch.shape[-1])
        part = jnp.dot(hid[i], w, preferred_element_type=f32)
        if i == 0:
            out[...] = part
        else:
            out[...] += part


def early(spot, mine, other, *groups):
    rows = mine.shape[0]
    depth, span = groups[0][0].shape
    return pl.pallas_call(
        early_body,
        out_shape=jax.ShapeDtypeStruct((rows, span), f32),
        in_specs=[SMEM] + [ANY] * 10,
        out_specs=VMEM,
        scratch_shapes=[
            pltpu.VMEM((8, depth, span), bf16),
            pltpu.VMEM((2,) + mine.shape, bf16),
            pltpu.SemaphoreType.DMA((2, 4)),
            pltpu.SemaphoreType.DMA((2,)),
        ],
        name="early",
    )(spot, mine, other, *[p for g in groups for p in g])


def late_body(spot, mine, other, acc, bias, gain, *refs):
    groups = [list(refs[:4]), list(refs[4:8])]
    scaled, squares = refs[8:10]
    scratch, hid, base, sems, hid_sems = refs[10:]
    waits = []
    for i, (one, zero) in enumerate(((mine, other), (other, mine))):
        copies = [pick_copy(spot[1], one, zero, hid.at[i], hid_sems.at[i])]
        pieces = place_square(spot[0], groups[i], scratch, sems.at[i], 4 * i)
        for c in pieces:
            c.start()
        waits.append(copies + pieces)
    load = pltpu.make_async_copy(acc, base, hid_sems.at[2])
    load.start()
    waits[1].append(load)
    span = base.shape[1]
    b = jnp.where(spot[2] == 1, bias[:, span:], bias[:, :span]).astype(f32)
    g = gain[0:1, :].astype(f32)
    for j in range(1, gain.shape[0]):
        g = jnp.where(spot[3] == j, gain[j : j + 1, :].astype(f32), g)
    for c in waits[0]:
        c.wait()
    before = jnp.dot(hid[0], scratch[0:4].reshape(-1, span), preferred_element_type=f32)
    for c in waits[1]:
        c.wait()
    base[...] += before
    w = scratch[4:8].reshape(-1, span)
    part = base.shape[0] // 4
    for i in range(4):
        at = slice(i * part, (i + 1) * part)
        total = base[at, :] + jnp.dot(hid[1, at, :], w, preferred_element_type=f32)
        projected = (total + b).astype(bf16).astype(f32)
        squares[at, :] = jnp.sum(projected * projected, axis=1, keepdims=True)
        scaled[at, :] = (projected * g).astype(bf16)


def late(spot, mine, other, acc, bias, gain, groups):
    rows, span = acc.shape
    depth = groups[0][0].shape[0]
    return pl.pallas_call(
        late_body,
        out_shape=[
            jax.ShapeDtypeStruct((rows, span), bf16),
            jax.ShapeDtypeStruct((rows, 1), f32),
        ],
        in_specs=[SMEM, ANY, ANY, ANY, VMEM, VMEM] + [ANY] * 8,
        out_specs=[VMEM] * 2,
        scratch_shapes=[
            pltpu.VMEM((8, depth, span), bf16),
            pltpu.VMEM((2,) + mine.shape, bf16),
            pltpu.VMEM((rows, span), f32),
            pltpu.SemaphoreType.DMA((2, 4)),
            pltpu.SemaphoreType.DMA((3,)),
        ],
        name="late",
    )(spot, mine, other, acc, bias, gain, *groups[0], *groups[1])


def kv_body(spot, scaled, p0, xu, xl, yu, yl, du, dl, own_keep, oth_keep, give, kv, kv_sems):
    copies = place_square(spot[0], [p0, (xu, xl), (yu, yl), (du, dl)], kv, kv_sems)
    for c in copies:
        c.start()
    for c in copies:
        c.wait()
    rows, half = own_keep.shape
    kv_rows = kv[...].reshape(-1, kv.shape[-1])
    for i in range(2):
        at = pl.ds(pl.multiple_of((spot[2] ^ i) * rows, rows), rows)
        got = jnp.dot(scaled[at, :], kv_rows, preferred_element_type=f32)
        left, right = got[:, :half], got[:, half:]
        (own_keep, oth_keep)[i][...] = jnp.where(spot[4] == 1, right, left)
        give[(1 - i) * rows : (2 - i) * rows, :] = jnp.where(spot[4] == 1, left, right).astype(bf16)


def kv_dot(spot, scaled, pieces):
    rows = scaled.shape[0]
    depth, width = pieces[0].shape
    keep = jax.ShapeDtypeStruct((rows // 2, width // 2), f32)
    return pl.pallas_call(
        kv_body,
        out_shape=[keep, keep, jax.ShapeDtypeStruct((rows, width // 2), bf16)],
        in_specs=[SMEM, VMEM] + [ANY] * 7,
        out_specs=[VMEM] * 3,
        scratch_shapes=[pltpu.VMEM((4, depth, width), bf16), pltpu.SemaphoreType.DMA((7,))],
        name="kv_dot",
    )(spot, scaled, *pieces)


def shards_square(
    encoded,
    frame_tokens,
    slot_owner,
    w_in,
    b_in,
    w_out,
    b_out,
    norm_gain,
    w_key,
    b_key,
    w_value,
    b_value,
):
    seq = lax.axis_size("seq")
    index = lax.axis_index("seq")
    core = lax.axis_index("mp")
    depth = seq.bit_length() - 1
    top, mate = depth - 1, depth - 2
    side = (index >> mate) & 1
    upper = (index >> top) & 1
    spot = jnp.stack(
        [index & 3, (upper == core).astype(jnp.int32), side, 2 * core + side, core, 2 * upper + side]
    )

    def send(x, *bits):
        flip = sum(1 << b for b in bits)
        return lax.ppermute(x, "seq", [(i, i ^ flip) for i in range(seq)])

    def some(x, pairs):
        return lax.ppermute(x, "seq", pairs)

    def halves(w):
        half = w.shape[1] // 2
        keep = lax.dynamic_slice_in_dim(w, side * half, half, 1)
        return keep, lax.dynamic_slice_in_dim(w, (1 - side) * half, half, 1)

    def square(own, over):
        x = send(own, 0)
        y = send(own, 1)
        return own, x, y, send((y, x)[over], over)

    in_keep, in_give = halves(w_in)
    out_keep, out_give = halves(w_out)
    in_e = send(in_give, mate)
    in_zk = send(in_keep, top)
    out_own = square(out_keep, 0)
    out_e = send(out_give, mate)
    in_ze = send(in_give, mate, top)
    kv = jnp.concatenate([w_key, w_value], axis=1)
    kv_row = join(kv, swap_core(kv), core, 1).reshape(kv.shape[0], -1)
    out_zk = send(out_keep, top)
    middle = [i for i in range(seq) if (i >> top ^ i >> mate) & 1 == 1]
    both_bits = (1 << top) | (1 << mate)
    near = some(out_give, [(i, i ^ both_bits) for i in middle])
    far_off = some(out_e, [(i, i ^ (1 << top)) for i in middle])
    out_ze = jnp.where(upper != side, near, far_off)
    quad = jnp.concatenate([in_keep, in_e, in_zk, in_ze])
    in_pieces = square(quad, 1)
    in_quads = [p.reshape((4,) + in_keep.shape) for p in in_pieces]
    out_from_e = square(out_e, 0)
    out_from_zk = square(out_zk, 1)
    out_from_ze = square(out_ze, 0)
    pairs = [
        (2 * i + h, 2 * (i ^ (1 << top)) + h) for i in range(seq) for h in range(2) if i >> top == h
    ]
    far = lax.ppermute(kv_row, ("seq", "mp"), pairs)
    kv_row = jnp.where(upper == core, kv_row, far)
    mid = kv_row.shape[0] // 2
    kv_u, kv_l = kv_row[:mid], kv_row[mid:]
    kv_xl = send(kv_l, 0)
    kv_yu = send(kv_u, 1)
    kv_xu = send(kv_u, 0)
    kv_yl = send(kv_l, 1)
    kv_du = send(kv_yu, 0)
    kv_dl = send(kv_xl, 1)
    kv_pieces = (kv_row, kv_xu, kv_xl, kv_yu, kv_yl, kv_du, kv_dl)

    rows, width = encoded.shape
    slots = 2 * seq
    rounds = rows // slots
    counts = frame_tokens[0]
    local = jnp.arange(rows, dtype=jnp.int32)
    frame = jnp.full((rows,), index * counts.shape[0], jnp.int32)
    begin = jnp.zeros((rows,), jnp.int32)
    end = 0
    for c in range(counts.shape[0]):
        end = end + counts[c]
        frame = frame + (end <= local).astype(jnp.int32)
        begin = begin + jnp.where(end <= local, counts[c], 0)
    offset = local - begin
    marks = jnp.stack([frame // 256, frame % 256, offset // 256, offset % 256], axis=1)
    marks = jnp.pad(marks.astype(bf16), ((0, 0), (0, LANE - 4)))
    tiles = width // LANE
    wide = (tiles + 1) // 2 * LANE
    low_half = encoded[:, :wide]
    second = jnp.concatenate([marks, encoded[:, wide:]], axis=1)
    if tiles % 2 == 0:
        low_half = jnp.pad(low_half, ((0, 0), (0, LANE)))
    payload = jnp.where(core == 1, second, low_half)
    slot = jnp.arange(slots, dtype=jnp.int32)
    same = (slot_owner[:, None] == slot_owner[None, :]) & (slot[None, :] < slot[:, None])
    place = slot_owner * (2 * rounds) + jnp.sum(same.astype(jnp.int32), axis=1)
    goal = (place[None, :] + 2 * jnp.arange(rounds, dtype=jnp.int32)[:, None]).reshape(-1)
    select = (local[:, None] == goal[None, :]).astype(bf16)
    moved = jnp.dot(select, payload, preferred_element_type=f32).astype(bf16)
    moved = moved.reshape(seq, 2 * rounds, -1)
    arrived = lax.all_to_all(moved, "seq", split_axis=0, concat_axis=0, tiled=True)
    arrived = arrived.reshape(rows, -1)
    other = swap_core(arrived)
    mate_rows = send(arrived, mate)
    own_tokens = (arrived, other, mate_rows, swap_core(mate_rows))
    own_marks = jnp.where(core == 1, arrived[:, :4], other[:, :4]).astype(f32)
    frame_ids = own_marks[:, 0] * 256 + own_marks[:, 1]
    offsets = own_marks[:, 2] * 256 + own_marks[:, 3]

    bias, gains = b_out[None, :], norm_gain.reshape(4, -1)
    hid = first(spot, own_tokens, in_quads, b_in[None, :], width, bias, gains)
    hid_c = swap_core(hid)
    hid_e = send(hid, mate)
    hid_ce = swap_core(hid_e)

    acc = early(spot, hid, hid_c, out_own, out_from_zk)
    scaled, squares = late(
        spot, hid_e, hid_ce, acc, bias, gains, (out_from_e, out_from_ze)
    )
    squares = squares[:, 0]
    squares = squares + swap_core(squares)
    squares = squares.reshape(2, rows)
    other_squares = send(jnp.where(side == 1, squares[0], squares[1]), mate)
    squares = jnp.where(side == 1, squares[1], squares[0]) + other_squares
    inv_rms = lax.rsqrt(squares / norm_gain.shape[0] + norm_eps)[:, None]
    own_keep, oth_keep, give = kv_dot(spot, scaled, kv_pieces)

    crossed = swap_core(give)
    oth_sum = (oth_keep + crossed[:rows].astype(f32)).astype(bf16)
    mate_sum = send(oth_sum, mate)
    summed = own_keep + crossed[rows:].astype(f32) + mate_sum.astype(f32)
    linear = summed * inv_rms
    half = w_key.shape[1]
    keys = rotate(linear[:, :half] + b_key.astype(f32), frame_ids, offsets).astype(bf16)
    vals = (linear[:, half:] + b_value.astype(f32)).astype(bf16)
    return keys, vals


def solution(mesh):
    square = mesh.shape["seq"] == 16
    return jax.shard_map(
        shards_square if square else shards,
        mesh=mesh,
        in_specs=(
            P("seq", None),
            P("seq", None),
            P(),
            P("seq", "mp"),
            P("mp"),
            P("seq", "mp"),
            P("mp"),
            P(),
            P("seq", "mp"),
            P("mp"),
            P("seq", "mp"),
            P("mp"),
        ),
        out_specs=(P("seq", "mp"), P("seq", "mp")),
        check_vma=False,
    )
```

```python
import jax
import jax.numpy as jnp
from jax import lax
from jax.experimental import pallas as pl
from jax.experimental.pallas import tpu as pltpu
from jax.sharding import PartitionSpec as P

HEAD = 128
TSEC = 16
LANE = 128

norm_eps = 1e-06
rope_base = 1000000.0


f32 = jnp.float32
bf16 = jnp.bfloat16


def rotate(linear, frame_ids, offsets):
    pairs = HEAD // 2
    pair_index = jnp.arange(pairs)
    inverse = jnp.power(f32(rope_base), -2.0 * pair_index.astype(f32) / HEAD)
    chosen = jnp.where(pair_index[None, :] < TSEC, frame_ids[:, None], offsets[:, None])
    angles = chosen * inverse[None, :]
    cosine = jnp.cos(angles)
    sine = jnp.sin(angles)
    turned = []
    for head in range(linear.shape[1] // HEAD):
        first = linear[:, head * HEAD : head * HEAD + pairs]
        second = linear[:, head * HEAD + pairs : (head + 1) * HEAD]
        turned += [first * cosine - second * sine, second * cosine + first * sine]
    return jnp.concatenate(turned, axis=1)


def swap(x, bit, count):
    return lax.ppermute(x, "seq", [(i, i ^ (1 << bit)) for i in range(count)])


def swap_core(x):
    return lax.ppermute(x, "mp", [(0, 1), (1, 0)])


def join(own, other, bit, axis):
    low = jnp.stack([own, other], axis=axis)
    high = jnp.stack([other, own], axis=axis)
    return jnp.where(bit == 1, high, low)


def spread(block, bits, held, values, count):
    held = list(held)
    for bit in bits:
        other = swap(block, bit, count)
        axis = sum(1 for b in held if b > bit)
        block = join(block, other, values[bit], axis)
        held.insert(axis, bit)
    return block.reshape(-1, block.shape[-1])


def cut_point(width):
    return (width // LANE + 1) // 2 * LANE


def shards(
    encoded,
    frame_tokens,
    slot_owner,
    w_in,
    b_in,
    w_out,
    b_out,
    norm_gain,
    w_key,
    b_key,
    w_value,
    b_value,
):
    seq = lax.axis_size("seq")
    index = lax.axis_index("seq")
    core = lax.axis_index("mp")
    depth = seq.bit_length() - 1
    assert seq == 1 << depth and lax.axis_size("mp") == 2
    values = [(index >> b) & 1 for b in range(depth)]
    top, mate = depth - 1, depth - 2
    lows = list(range(depth - 2))
    orders = (lows, lows[::-1])
    side = values[mate]

    def halves(w):
        half = w.shape[1] // 2
        left, right = w[:, :half], w[:, half:]
        return jnp.where(side == 1, right, left), jnp.where(side == 1, left, right)

    def gather(w):
        keep, give = halves(w)
        pair = join(keep, swap(give, mate, seq), side, 0)
        quad = join(pair, swap(pair, top, seq), values[top], 0)
        cut = cut_point(keep.shape[1])
        parts = (quad[..., :cut], quad[..., cut:])
        return [spread(p, o, (top, mate), values, seq) for p, o in zip(parts, orders)]

    rows, width = encoded.shape
    slots = 2 * seq
    rounds = rows // slots
    counts = frame_tokens[0]
    local = jnp.arange(rows, dtype=jnp.int32)
    ends = jnp.cumsum(counts)
    done = ends[None, :] <= local[:, None]
    frame = index * counts.shape[0] + jnp.sum(done.astype(jnp.int32), axis=1)
    offset = local - jnp.sum(jnp.where(done, counts[None, :], 0), axis=1)
    marks = jnp.stack([frame // 256, frame % 256, offset // 256, offset % 256], axis=1)
    marks = jnp.pad(marks.astype(bf16), ((0, 0), (0, LANE - 4)))
    tiles = width // LANE
    wide = (tiles + 1) // 2 * LANE
    first = encoded[:, :wide]
    second = jnp.concatenate([marks, encoded[:, wide:]], axis=1)
    if second.shape[1] < wide + (LANE if tiles % 2 == 0 else 0):
        raise ValueError("width")
    if tiles % 2 == 0:
        first = jnp.pad(first, ((0, 0), (0, LANE)))
    payload = jnp.where(core == 1, second, first)
    order = jnp.argsort(slot_owner, stable=True).astype(jnp.int32)
    pick = (
        jnp.arange(rounds, dtype=jnp.int32)[None, :, None] * slots + order.reshape(seq, 1, 2)
    ).reshape(-1)
    moved = jnp.take(payload, pick, axis=0).reshape(seq, 2 * rounds, -1)
    arrived = lax.all_to_all(moved, "seq", split_axis=0, concat_axis=0, tiled=True)
    arrived = arrived.reshape(rows, -1)
    both = join(arrived, swap(arrived, mate, seq), side, 0).reshape(2 * rows, -1)
    ready = join(both, swap_core(both), core, 0)
    tokens = jnp.concatenate([ready[0, :, :wide], ready[1, :, LANE:]], axis=1)
    own_marks = lax.dynamic_slice_in_dim(ready[1, :, :4], side * rows, rows, 0).astype(f32)
    frame_ids = own_marks[:, 0] * 256 + own_marks[:, 1]
    offsets = own_marks[:, 2] * 256 + own_marks[:, 3]

    own_b_in, _ = halves(b_in[None, :])
    cut = cut_point(own_b_in.shape[1])
    hidden = []
    for w, b in zip(gather(w_in), (own_b_in[:, :cut], own_b_in[:, cut:])):
        pre = jnp.dot(tokens, w, preferred_element_type=f32) + b.astype(f32)
        part = jax.nn.gelu(pre, approximate=False).astype(bf16)
        hidden.append(part)
    quarter = jnp.concatenate(hidden, axis=1)
    pair_hidden = join(quarter, swap(quarter, mate, seq), side, 0)
    all_hidden = join(pair_hidden, swap_core(pair_hidden), core, 0)
    all_hidden = all_hidden.reshape((4,) + quarter.shape)

    kv = jnp.concatenate([w_key, w_value], axis=1)
    kv_row = join(kv, swap_core(kv), core, 1).reshape(kv.shape[0], -1)
    pairs = [
        (2 * i + h, 2 * (i ^ (1 << top)) + h) for i in range(seq) for h in range(2) if i >> top == h
    ]
    far = lax.ppermute(kv_row, ("seq", "mp"), pairs)
    kv_row = jnp.where(values[top] == core, kv_row, far)
    kv_cut = kv_row.shape[1] // 2
    kv_full = jnp.concatenate(
        [
            spread(p, o, (), values, seq)
            for p, o in zip((kv_row[:, :kv_cut], kv_row[:, kv_cut:]), orders)
        ],
        axis=1,
    )

    own_b_out, _ = halves(b_out[None, :])
    span = own_b_out.shape[1]
    gain = lax.dynamic_slice_in_dim(norm_gain, (2 * core + side) * span, span)[None, :]
    squares = 0.0
    partial = 0.0
    start = 0
    for w in gather(w_out):
        stop = start + w.shape[1]
        blocks = w.reshape(4, -1, w.shape[1])
        summed = own_b_out[:, start:stop].astype(f32)
        for q in range(4):
            summed = summed + jnp.dot(all_hidden[q], blocks[q], preferred_element_type=f32)
        projected = summed.astype(bf16).astype(f32)
        squares = squares + jnp.sum(projected * projected, axis=1)
        scaled = (projected * gain[:, start:stop].astype(f32)).astype(bf16)
        partial = partial + jnp.dot(scaled, kv_full[start:stop], preferred_element_type=f32)
        start = stop

    squares = squares + swap_core(squares)
    squares = squares.reshape(2, rows)
    other_squares = swap(jnp.where(side == 1, squares[0], squares[1]), mate, seq)
    squares = jnp.where(side == 1, squares[1], squares[0]) + other_squares
    inv_rms = lax.rsqrt(squares / norm_gain.shape[0] + norm_eps)[:, None]

    keep = jnp.where(core == 1, partial[:, kv_cut:], partial[:, :kv_cut])
    give = jnp.where(core == 1, partial[:, :kv_cut], partial[:, kv_cut:])
    summed = keep + swap_core(give)
    keep = jnp.where(side == 1, summed[rows:], summed[:rows])
    give = jnp.where(side == 1, summed[:rows], summed[rows:])
    summed = keep + swap(give.astype(bf16), mate, seq).astype(f32)
    linear = summed * inv_rms
    half = w_key.shape[1]
    keys = rotate(linear[:, :half] + b_key.astype(f32), frame_ids, offsets).astype(bf16)
    vals = (linear[:, half:] + b_value.astype(f32)).astype(bf16)
    return keys, vals


ANY = pl.BlockSpec(memory_space=pl.ANY)
VMEM = pl.BlockSpec(memory_space=pltpu.VMEM)
SMEM = pl.BlockSpec(memory_space=pltpu.SMEM)


def place_square(where, pieces, scratch, sems, base=0):
    copies = []
    for d, block in enumerate(pieces):
        parts = block if isinstance(block, tuple) else (block,)
        at = 0
        for part in parts:
            spot = scratch.at[base + (where ^ d)]
            if len(parts) > 1:
                spot = scratch.at[base + (where ^ d), pl.ds(at, part.shape[0])]
            at += part.shape[0]
            copies.append(pltpu.make_async_copy(part, spot, sems.at[len(copies)]))
    return copies


def pick_copy(flag, one, zero, spot, sem):
    @pl.when(flag == 1)
    def _():
        pltpu.make_async_copy(one, spot, sem).start()

    @pl.when(flag == 0)
    def _():
        pltpu.make_async_copy(zero, spot, sem).start()

    return pltpu.make_async_copy(one, spot, sem)


def first_body(spot, *refs):
    mine, other, mate, mate_other = refs[:4]
    quads = refs[4:8]
    bias = refs[8]
    out, tokens, w, sems, tok_sems = refs[-5:]
    rows, wide = mine.shape
    rest = tokens.shape[1] - wide
    waits = []
    for d, quad in enumerate(quads):
        for z in range(4):
            place = w.at[(spot[5] ^ z) * 4 + (spot[0] ^ d)]
            waits.append(pltpu.make_async_copy(quad.at[z], place, sems.at[d, z]))
    for c in waits:
        c.start()
    skip = wide - rest
    for i, (one, zero) in enumerate(((mine, other), (mate, mate_other))):
        at = pl.ds(pl.multiple_of((spot[2] ^ i) * rows, rows), rows)
        low, high = tokens.at[at, pl.ds(0, wide)], tokens.at[at, pl.ds(wide, rest)]
        cut = pl.ds(skip, rest)
        waits.append(pick_copy(spot[4], zero, one, low, tok_sems.at[i, 0]))
        waits.append(
            pick_copy(spot[4], one.at[:, cut], zero.at[:, cut], high, tok_sems.at[i, 1])
        )
    for c in waits:
        c.wait()
    weights = w[...].reshape(-1, w.shape[-1])
    span = weights.shape[1]
    b = jnp.where(spot[2] == 1, bias[:, span:], bias[:, :span]).astype(f32)
    part = rows // 2
    for i in range(4):
        at = slice(i * part, (i + 1) * part)
        pre = jnp.dot(tokens[at, :], weights, preferred_element_type=f32) + b
        out[at, :] = (0.5 * pre * (1.0 + lax.erf(pre * (0.5**0.5)))).astype(bf16)


def first(spot, own, quads, bias, width, *unused):
    rows, _ = own[0].shape
    span = quads[0].shape[-1]
    return pl.pallas_call(
        first_body,
        out_shape=jax.ShapeDtypeStruct((2 * rows, span), bf16),
        in_specs=[SMEM] + [ANY] * 8 + [VMEM] + [ANY] * len(unused),
        out_specs=VMEM,
        scratch_shapes=[
            pltpu.VMEM((2 * rows, width), bf16),
            pltpu.VMEM((16,) + quads[0].shape[1:], bf16),
            pltpu.SemaphoreType.DMA((4, 4)),
            pltpu.SemaphoreType.DMA((2, 2)),
        ],
        name="first",
    )(spot, *own, *quads, bias, *unused)


def early_body(spot, mine, other, *refs):
    groups = [list(refs[4 * i : 4 * i + 4]) for i in range(2)]
    out, scratch, hid, sems, hid_sems = refs[8:]
    waits = []
    for i, (one, zero) in enumerate(((mine, other), (other, mine))):
        copies = [pick_copy(spot[1], one, zero, hid.at[i], hid_sems.at[i])]
        pieces = place_square(spot[0], groups[i], scratch, sems.at[i], 4 * i)
        for c in pieces:
            c.start()
        waits.append(copies + pieces)
    for i in range(2):
        for c in waits[i]:
            c.wait()
        w = scratch[4 * i : 4 * i + 4].reshape(-1, scratch.shape[-1])
        part = jnp.dot(hid[i], w, preferred_element_type=f32)
        if i == 0:
            out[...] = part
        else:
            out[...] += part


def early(spot, mine, other, *groups):
    rows = mine.shape[0]
    depth, span = groups[0][0].shape
    return pl.pallas_call(
        early_body,
        out_shape=jax.ShapeDtypeStruct((rows, span), f32),
        in_specs=[SMEM] + [ANY] * 10,
        out_specs=VMEM,
        scratch_shapes=[
            pltpu.VMEM((8, depth, span), bf16),
            pltpu.VMEM((2,) + mine.shape, bf16),
            pltpu.SemaphoreType.DMA((2, 4)),
            pltpu.SemaphoreType.DMA((2,)),
        ],
        name="early",
    )(spot, mine, other, *[p for g in groups for p in g])


def late_body(spot, mine, other, acc, bias, gain, *refs):
    groups = [list(refs[:4]), list(refs[4:8])]
    scaled, squares = refs[8:10]
    scratch, hid, base, sems, hid_sems = refs[10:]
    waits = []
    for i, (one, zero) in enumerate(((mine, other), (other, mine))):
        copies = [pick_copy(spot[1], one, zero, hid.at[i], hid_sems.at[i])]
        pieces = place_square(spot[0], groups[i], scratch, sems.at[i], 4 * i)
        for c in pieces:
            c.start()
        waits.append(copies + pieces)
    load = pltpu.make_async_copy(acc, base, hid_sems.at[2])
    load.start()
    waits[1].append(load)
    span = base.shape[1]
    b = jnp.where(spot[2] == 1, bias[:, span:], bias[:, :span]).astype(f32)
    g = gain[0:1, :].astype(f32)
    for j in range(1, gain.shape[0]):
        g = jnp.where(spot[3] == j, gain[j : j + 1, :].astype(f32), g)
    for c in waits[0]:
        c.wait()
    before = jnp.dot(hid[0], scratch[0:4].reshape(-1, span), preferred_element_type=f32)
    for c in waits[1]:
        c.wait()
    base[...] += before
    w = scratch[4:8].reshape(-1, span)
    part = base.shape[0] // 4
    for i in range(4):
        at = slice(i * part, (i + 1) * part)
        total = base[at, :] + jnp.dot(hid[1, at, :], w, preferred_element_type=f32)
        projected = (total + b).astype(bf16).astype(f32)
        squares[at, :] = jnp.sum(projected * projected, axis=1, keepdims=True)
        scaled[at, :] = (projected * g).astype(bf16)


def late(spot, mine, other, acc, bias, gain, groups):
    rows, span = acc.shape
    depth = groups[0][0].shape[0]
    return pl.pallas_call(
        late_body,
        out_shape=[
            jax.ShapeDtypeStruct((rows, span), bf16),
            jax.ShapeDtypeStruct((rows, 1), f32),
        ],
        in_specs=[SMEM, ANY, ANY, ANY, VMEM, VMEM] + [ANY] * 8,
        out_specs=[VMEM] * 2,
        scratch_shapes=[
            pltpu.VMEM((8, depth, span), bf16),
            pltpu.VMEM((2,) + mine.shape, bf16),
            pltpu.VMEM((rows, span), f32),
            pltpu.SemaphoreType.DMA((2, 4)),
            pltpu.SemaphoreType.DMA((3,)),
        ],
        name="late",
    )(spot, mine, other, acc, bias, gain, *groups[0], *groups[1])


def kv_body(spot, scaled, p0, xu, xl, yu, yl, du, dl, own_keep, oth_keep, give, kv, kv_sems):
    copies = place_square(spot[0], [p0, (xu, xl), (yu, yl), (du, dl)], kv, kv_sems)
    for c in copies:
        c.start()
    for c in copies:
        c.wait()
    rows, half = own_keep.shape
    kv_rows = kv[...].reshape(-1, kv.shape[-1])
    for i in range(2):
        at = pl.ds(pl.multiple_of((spot[2] ^ i) * rows, rows), rows)
        got = jnp.dot(scaled[at, :], kv_rows, preferred_element_type=f32)
        left, right = got[:, :half], got[:, half:]
        (own_keep, oth_keep)[i][...] = jnp.where(spot[4] == 1, right, left)
        give[(1 - i) * rows : (2 - i) * rows, :] = jnp.where(spot[4] == 1, left, right).astype(bf16)


def kv_dot(spot, scaled, pieces):
    rows = scaled.shape[0]
    depth, width = pieces[0].shape
    keep = jax.ShapeDtypeStruct((rows // 2, width // 2), f32)
    return pl.pallas_call(
        kv_body,
        out_shape=[keep, keep, jax.ShapeDtypeStruct((rows, width // 2), bf16)],
        in_specs=[SMEM, VMEM] + [ANY] * 7,
        out_specs=[VMEM] * 3,
        scratch_shapes=[pltpu.VMEM((4, depth, width), bf16), pltpu.SemaphoreType.DMA((7,))],
        name="kv_dot",
    )(spot, scaled, *pieces)


def shards_square(
    encoded,
    frame_tokens,
    slot_owner,
    w_in,
    b_in,
    w_out,
    b_out,
    norm_gain,
    w_key,
    b_key,
    w_value,
    b_value,
):
    seq = lax.axis_size("seq")
    index = lax.axis_index("seq")
    core = lax.axis_index("mp")
    depth = seq.bit_length() - 1
    top, mate = depth - 1, depth - 2
    side = (index >> mate) & 1
    upper = (index >> top) & 1
    spot = jnp.stack(
        [index & 3, (upper == core).astype(jnp.int32), side, 2 * core + side, core, 2 * upper + side]
    )

    def send(x, *bits):
        flip = sum(1 << b for b in bits)
        return lax.ppermute(x, "seq", [(i, i ^ flip) for i in range(seq)])

    def some(x, pairs):
        return lax.ppermute(x, "seq", pairs)

    def halves(w):
        half = w.shape[1] // 2
        keep = lax.dynamic_slice_in_dim(w, side * half, half, 1)
        return keep, lax.dynamic_slice_in_dim(w, (1 - side) * half, half, 1)

    def square(own, over):
        x = send(own, 0)
        y = send(own, 1)
        return own, x, y, send((y, x)[over], over)

    in_keep, in_give = halves(w_in)
    out_keep, out_give = halves(w_out)
    in_e = send(in_give, mate)
    in_zk = send(in_keep, top)
    out_own = square(out_keep, 0)
    out_e = send(out_give, mate)
    bias_in, bias, gains = b_in[None, :], b_out[None, :], norm_gain.reshape(4, -1)
    out_e, bias_in, bias, gains, spot = lax.optimization_barrier(
        (out_e, bias_in, bias, gains, spot)
    )
    in_ze = send(in_give, mate, top)
    kv = jnp.concatenate([w_key, w_value], axis=1)
    kv_row = join(kv, swap_core(kv), core, 1).reshape(kv.shape[0], -1)
    out_zk = send(out_keep, top)
    middle = [i for i in range(seq) if (i >> top ^ i >> mate) & 1 == 1]
    both_bits = (1 << top) | (1 << mate)
    near = some(out_give, [(i, i ^ both_bits) for i in middle])
    far_off = some(out_e, [(i, i ^ (1 << top)) for i in middle])
    out_ze = jnp.where(upper != side, near, far_off)
    quad = jnp.concatenate([in_keep, in_e, in_zk, in_ze])
    in_pieces = square(quad, 1)
    in_quads = [p.reshape((4,) + in_keep.shape) for p in in_pieces]
    out_from_e = square(out_e, 0)
    out_from_zk = square(out_zk, 1)
    out_from_ze = square(out_ze, 0)
    pairs = [
        (2 * i + h, 2 * (i ^ (1 << top)) + h) for i in range(seq) for h in range(2) if i >> top == h
    ]
    far = lax.ppermute(kv_row, ("seq", "mp"), pairs)
    kv_row = jnp.where(upper == core, kv_row, far)
    mid = kv_row.shape[0] // 2
    kv_u, kv_l = kv_row[:mid], kv_row[mid:]
    kv_xl = send(kv_l, 0)
    kv_yu = send(kv_u, 1)
    kv_xu = send(kv_u, 0)
    kv_yl = send(kv_l, 1)
    kv_du = send(kv_yu, 0)
    kv_dl = send(kv_xl, 1)
    kv_pieces = (kv_row, kv_xu, kv_xl, kv_yu, kv_yl, kv_du, kv_dl)

    rows, width = encoded.shape
    slots = 2 * seq
    rounds = rows // slots
    counts = frame_tokens[0]
    local = jnp.arange(rows, dtype=jnp.int32)
    frame = jnp.full((rows,), index * counts.shape[0], jnp.int32)
    begin = jnp.zeros((rows,), jnp.int32)
    end = 0
    for c in range(counts.shape[0]):
        end = end + counts[c]
        frame = frame + (end <= local).astype(jnp.int32)
        begin = begin + jnp.where(end <= local, counts[c], 0)
    offset = local - begin
    marks = jnp.stack([frame // 256, frame % 256, offset // 256, offset % 256], axis=1)
    marks = jnp.pad(marks.astype(bf16), ((0, 0), (0, LANE - 4)))
    tiles = width // LANE
    wide = (tiles + 1) // 2 * LANE
    low_half = encoded[:, :wide]
    second = jnp.concatenate([marks, encoded[:, wide:]], axis=1)
    if tiles % 2 == 0:
        low_half = jnp.pad(low_half, ((0, 0), (0, LANE)))
    payload = jnp.where(core == 1, second, low_half)
    slot = jnp.arange(slots, dtype=jnp.int32)
    same = (slot_owner[:, None] == slot_owner[None, :]) & (slot[None, :] < slot[:, None])
    place = slot_owner * (2 * rounds) + jnp.sum(same.astype(jnp.int32), axis=1)
    goal = (place[None, :] + 2 * jnp.arange(rounds, dtype=jnp.int32)[:, None]).reshape(-1)
    select = (local[:, None] == goal[None, :]).astype(bf16)
    moved = jnp.dot(select, payload, preferred_element_type=f32).astype(bf16)
    moved = moved.reshape(seq, 2 * rounds, -1)
    arrived = lax.all_to_all(moved, "seq", split_axis=0, concat_axis=0, tiled=True)
    arrived = arrived.reshape(rows, -1)
    other = swap_core(arrived)
    mate_rows = send(arrived, mate)
    own_tokens = (arrived, other, mate_rows, swap_core(mate_rows))
    own_marks = jnp.where(core == 1, arrived[:, :4], other[:, :4]).astype(f32)
    frame_ids = own_marks[:, 0] * 256 + own_marks[:, 1]
    offsets = own_marks[:, 2] * 256 + own_marks[:, 3]

    hid = first(spot, own_tokens, in_quads, bias_in, width)
    hid_c = swap_core(hid)
    hid_e = send(hid, mate)
    hid_ce = swap_core(hid_e)

    acc = early(spot, hid, hid_c, out_own, out_from_zk)
    acc, frame_ids, offsets = lax.optimization_barrier((acc, frame_ids, offsets))
    scaled, squares = late(
        spot, hid_e, hid_ce, acc, bias, gains, (out_from_e, out_from_ze)
    )
    squares = squares[:, 0]
    squares = squares + swap_core(squares)
    squares = squares.reshape(2, rows)
    other_squares = send(jnp.where(side == 1, squares[0], squares[1]), mate)
    squares = jnp.where(side == 1, squares[1], squares[0]) + other_squares
    inv_rms = lax.rsqrt(squares / norm_gain.shape[0] + norm_eps)[:, None]
    own_keep, oth_keep, give = kv_dot(spot, scaled, kv_pieces)

    crossed = swap_core(give)
    oth_sum = (oth_keep + crossed[:rows].astype(f32)).astype(bf16)
    mate_sum = send(oth_sum, mate)
    summed = own_keep + crossed[rows:].astype(f32) + mate_sum.astype(f32)
    linear = summed * inv_rms
    half = w_key.shape[1]
    keys = rotate(linear[:, :half] + b_key.astype(f32), frame_ids, offsets).astype(bf16)
    vals = (linear[:, half:] + b_value.astype(f32)).astype(bf16)
    return keys, vals


def solution(mesh):
    square = mesh.shape["seq"] == 16
    return jax.shard_map(
        shards_square if square else shards,
        mesh=mesh,
        in_specs=(
            P("seq", None),
            P("seq", None),
            P(),
            P("seq", "mp"),
            P("mp"),
            P("seq", "mp"),
            P("mp"),
            P(),
            P("seq", "mp"),
            P("mp"),
            P("seq", "mp"),
            P("mp"),
        ),
        out_specs=(P("seq", "mp"), P("seq", "mp")),
        check_vma=False,
    )
```
